256 devices in a mesh: curve: 32 (over x, z), grp: 8 (over y, core).
Axes of the slice: x: 4, y: 4, z: 8, core: 2. Of those that a mesh axis runs over, the one named last changes fastest.
Arguments:
- state: float32 [2, 512, 8, 49152], P(None, None, 'grp', 'curve'), may hold values from -6 to 6
- coef: float32 [512, 8, 49152], P(None, 'grp', 'curve'), may hold values from 0.2 to 4
- counts: int32 [8, 32], P('grp', 'curve'), may hold values from 512 to 1536, as said below
Outputs:
- smoothed: float32 [512, 8, 32768], P(None, 'grp', 'curve')
The draws below stay inside these ranges and needn't reach their ends.
Inputs may be any that keep to these rules, and one draw needn't show every extreme that they name: `counts`: each rank's count is 1024 plus the drift at its own end minus the drift at the end of the rank before it; drifts lie in -256 to 256, are zero before the first rank and at the last rank, so the curve holds 32768 blocks; in every curve one rank holds exactly 1536 blocks.
All inputs are finite; a program needn't handle non-finite values.
Results may differ from the reference program's by a relative error of at most 0.00002.
Values sent between devices are 32-bit elements; how exact they have to be, the bound alone decides.
A program may use at most 128 MiB of HBM per device.

```python
import math
import jax
import jax.numpy as jnp

AVG = 1024
HALF = 256
CAP = 1536
SWEEPS = 2
N_CURVE = 32
N_GRP = 8


def draw_counts(key, part):
    key_walk, key_peak = jax.random.split(jax.random.fold_in(key, 11))
    drift = jax.random.randint(key_walk, (N_GRP, N_CURVE), -HALF, HALF + 1)
    peak = jax.random.randint(key_peak, (N_GRP, 1), 1, N_CURVE - 1)
    column = jnp.arange(N_CURVE, dtype=jnp.int32)[None, :]
    drift = jnp.where(column == peak, HALF, jnp.where(column == peak - 1, -HALF, drift))
    drift = jnp.where(column == N_CURVE - 1, 0, drift)
    before = jnp.concatenate([jnp.zeros((N_GRP, 1), jnp.int32), drift[:, :-1]], axis=1)
    return (AVG + drift - before).astype(jnp.int32)


def block_scale(stream_key, extent, pieces, smallest, high):
    loudness, own = 1.0, jax.random.fold_in(stream_key, 6)
    for axis_at, shards_of in pieces:
        draws = jnp.exp(jax.random.uniform(jax.random.fold_in(own, axis_at), (shards_of,), jnp.float32, smallest / len(pieces), high / len(pieces)))
        loudness = loudness * jnp.repeat(draws, extent[axis_at] // shards_of).reshape([-1 if axis == axis_at else 1 for axis in range(len(extent))])
    return loudness


def gaussian(key, dims, scale, limit, pieces=(), held_as=jnp.bfloat16):
    level = block_scale(key, dims, pieces, -0.22, 0.18) if pieces else 1.0
    values = jax.random.normal(key, dims, jnp.float32) * scale * level
    return jnp.minimum(jnp.maximum(values, -limit), limit).astype(held_as)


def setup_inputs(seed: int = 0) -> dict:
    key_list = jax.random.split(jax.random.key(seed), 4)
    return {
        "state": gaussian(key_list[0], (2, 512, N_GRP, N_CURVE * CAP), 1.0, 6.0, ((2, 8), (3, 32)), jnp.float32),
        "coef": jnp.clip(jnp.exp(math.log(4.0) - 2.9957323 * jax.random.uniform(key_list[1], (512, N_GRP, N_CURVE * CAP), jnp.float32) ** block_scale(key_list[1], (512, N_GRP, N_CURVE * CAP), ((1, 8), (2, 32)), -0.2, 0.2)), 0.2, 4.0),
        "counts": draw_counts(jax.random.fold_in(key_list[3], 71), 0),
    }


def smooth(field, source, coef, left_block, right_block, low_face, high_face):
    xplus = jnp.concatenate([field[1:], jnp.concatenate([field[0:1, :, :, :, 1:], right_block[0:1]], axis=4)], axis=0)
    xminus = jnp.concatenate([jnp.concatenate([left_block[7:8], field[7:8, :, :, :, :-1]], axis=4), field[:-1]], axis=0)
    yplus = jnp.concatenate([field[:, 1:], high_face[:, None]], axis=1)
    yminus = jnp.concatenate([low_face[:, None], field[:, :-1]], axis=1)
    zeroes = jnp.zeros_like(field[:, :, 0:1])
    zplus = jnp.concatenate([field[:, :, 1:], zeroes], axis=2)
    zminus = jnp.concatenate([zeroes, field[:, :, :-1]], axis=2)
    total = xplus + xminus + yplus + yminus + zplus + zminus
    return (source + total) / (6.0 + coef)


def reference(state, coef, counts):
    prefix = jnp.cumsum(counts, axis=1) - counts
    blocks = N_CURVE * AVG
    target = jnp.arange(blocks, dtype=jnp.int32)
    owner = jnp.sum((prefix[:, None, :] <= target[None, :, None]).astype(jnp.int32), axis=2) - 1
    start = jnp.take_along_axis(prefix, owner, axis=1)
    source_col = (owner * CAP + target[None, :] - start).astype(jnp.int32)
    moved = jnp.take_along_axis(state, jnp.broadcast_to(source_col[None, None], (2, 512, N_GRP, blocks)), axis=3)
    moved_coef = jnp.take_along_axis(coef, jnp.broadcast_to(source_col[None], (512, N_GRP, blocks)), axis=2)
    field = moved[0].reshape(8, 8, 8, N_GRP, blocks)
    source = moved[1].reshape(8, 8, 8, N_GRP, blocks)
    cellcoef = moved_coef.reshape(8, 8, 8, N_GRP, blocks)
    edge = jnp.zeros((8, 8, 8, N_GRP, 1), jnp.float32)
    plane = jnp.zeros((8, 8, 1, blocks), jnp.float32)
    for sweep in range(SWEEPS):
        low_face = jnp.concatenate([plane, field[:, 7, :, :-1, :]], axis=2)
        high_face = jnp.concatenate([field[:, 0, :, 1:, :], plane], axis=2)
        field = smooth(field, source, cellcoef, edge, edge, low_face, high_face)
    return field.reshape(512, N_GRP, blocks)
```

```python
import jax
import jax.numpy as jnp
from jax import lax
from jax.experimental import pallas as pl
from jax.experimental.pallas import tpu as pltpu
from jax.sharding import PartitionSpec as P

AVG = 1024
HALF = 256
CAP = 1536
NX, NZ = 4, 8
N_CURVE = NX * NZ
N_GRP = 8
CH = CAP // 128
MESH = pl.DeviceIdType.MESH
ORDER = (2, 3, 4, 5, 1, 6, 0, 7)
GROUPS = ((0, 4), (4, 2), (6, 2))


class Message:
    def __init__(self, make, sends, receives):
        self.make, self.sends, self.receives = make, sends, receives

    def start(self):
        pl.when(self.sends)(lambda: self.make().start())

    def wait_recv(self):
        pl.when(self.receives)(lambda: self.make().wait_recv())

    def wait_send(self):
        pl.when(self.sends)(lambda: self.make().wait_send())


def kernel(
    counts, state, coef, out,
    raw_u, raw_s, raw_c, u0, u1, inv, yh, rx0, rx1, ts0, ts1, ps, pr, ls, lr,
    t2s, t2r, h2s, h2r, wide, flat, cb1, cb2, cb3, cs,
    in_sem, out_sem, send_sem, recv_sem,
):
    rank, grp = lax.axis_index("curve"), lax.axis_index("grp")
    xc, zc = rank // NZ, rank % NZ
    has_left, has_right = rank > 0, rank < N_CURVE - 1
    has_low, has_high = grp > 0, grp < N_GRP - 1
    left, right = (rank + N_CURVE - 1) % N_CURVE, (rank + 1) % N_CURVE
    low, high = (grp + N_GRP - 1) % N_GRP, (grp + 1) % N_GRP

    barrier = pltpu.get_barrier_semaphore()
    peers = [(xc * NZ + (zc + k) % NZ, grp) for k in range(1, NZ)]
    peers += [(((xc + k) % NX) * NZ + zc, grp) for k in range(1, NX)]
    peers += [(r, g) for g in (low, high) for r in (left, rank, right)]
    peers += [(left, grp), (right, grp)]
    for peer in peers:
        pl.semaphore_signal(barrier, inc=1, device_id=peer, device_id_type=MESH)

    loads = {}
    for kind, src, dst in ((0, state.at[0], raw_u), (1, state.at[1], raw_s), (2, coef, raw_c)):
        for x in range(8):
            loads[kind, x] = pltpu.make_async_copy(src.at[x], dst.at[x], in_sem.at[kind, x])
    first_loads = [(0, x) for x in range(8)] + [(1, 0), (1, 7), (2, 0), (2, 7)]
    other_loads = [(kind, x) for x in range(1, 7) for kind in (1, 2)]
    for key in first_loads + other_loads:
        loads[key].start()

    lane = lax.broadcasted_iota(jnp.int32, (8, 128), 1)
    sub = lax.broadcasted_iota(jnp.int32, (8, 128), 0)
    zero = jnp.zeros((8, 128), jnp.float32)
    held = counts[0, 0]

    index = [0]

    def message(src, dst, device, sends, receives):
        at = index[0]
        index[0] += 1

        def make():
            return pltpu.make_async_remote_copy(
                src_ref=src(), dst_ref=dst(), send_sem=send_sem.at[at], recv_sem=recv_sem.at[at],
                device_id=device, device_id_type=MESH,
            )

        return Message(make, sends, receives)

    yes = rank >= 0
    count_z = [
        message(lambda: cs.at[0], lambda: cb1.at[zc], (xc * NZ + (zc + k) % NZ, grp), yes, yes)
        for k in range(1, NZ)
    ]
    count_x = [
        message(lambda: cs.at[1], lambda: cb2.at[xc], (((xc + k) % NX) * NZ + zc, grp), yes, yes)
        for k in range(1, NX)
    ]
    count_g = [
        message(lambda: cs.at[2], lambda: cb3.at[1], (rank, low), has_low, has_high),
        message(lambda: cs.at[2], lambda: cb3.at[0], (rank, high), has_high, has_low),
    ]
    packs = [
        message(lambda: ps.at[0], lambda: pr.at[1], (left, grp), has_left, has_right),
        message(lambda: ps.at[1], lambda: pr.at[0], (right, grp), has_right, has_left),
    ]
    late_packs = [
        message(lambda: ls.at[0], lambda: lr.at[1], (left, grp), has_left, has_right),
        message(lambda: ls.at[1], lambda: lr.at[0], (right, grp), has_right, has_left),
    ]

    def planes_out(u, ts, rx):
        tails, heads, mids = [], [], []
        for d, y, other, sends, receives in (
            (0, 0, low, has_low, has_high), (1, 7, high, has_high, has_low),
        ):
            tails.append(message(
                lambda d=d: ts.at[d], lambda d=d: rx.at[1 - d, :, pl.ds(0, 4)], (right, other),
                jnp.logical_and(sends, has_right), jnp.logical_and(receives, has_left)))
            heads.append(message(
                lambda y=y: u.at[pl.ds(1, 8), y, pl.ds(0, 4)],
                lambda d=d: rx.at[1 - d, :, pl.ds(16, 4)], (left, other),
                jnp.logical_and(sends, has_left), jnp.logical_and(receives, has_right)))
            mids.append(message(
                lambda y=y: u.at[pl.ds(1, 8), y], lambda d=d: rx.at[1 - d, :, pl.ds(4, 12)],
                (rank, other), sends, receives))
        return tails + heads + mids

    planes0 = planes_out(u0, ts0, rx0)
    planes1 = planes_out(u1, ts1, rx1)
    moves = []
    for start, size in GROUPS:
        part = pl.ds(start, size)
        moves.append([
            message(lambda part=part: t2s.at[part], lambda part=part: t2r.at[part], (right, grp),
                    has_right, has_left),
            message(lambda part=part: h2s.at[part], lambda part=part: h2r.at[part], (left, grp),
                    has_left, has_right),
        ])

    def rolled(value, turn):
        return pltpu.roll(value, turn, 1)

    def shifted(load, start, chunks, lowest, highest):
        first, offset = jnp.clip(start >> 7, lowest, highest), start & 127
        turn = (128 - offset) & 127
        turned = {}
        for k in sorted(set(chunks) | {k + 1 for k in chunks}):
            turned[k] = rolled(load(first + k), turn)
        keep = lane < 128 - offset
        return {k: jnp.where(keep, turned[k], turned[k + 1]) for k in chunks}

    def convert(x, carry):
        for y in range(8):
            for c in range(CH):
                u0[x + 1, y, c] = raw_u[x, y, pl.ds(c, 8, stride=CH), :]
        return carry

    def plane_tails(u, ts):
        def body(x, carry):
            for d, y in ((0, 0), (1, 7)):
                got = shifted(
                    lambda k: u[x + 1, y, jnp.minimum(k, CH - 1)], held - 512, range(4), 0, 8)
                for k in range(4):
                    ts[d, x, k] = got[k]
            return carry

        lax.fori_loop(0, 8, body, 0)

    last_chunk, last_lane = jnp.clip((held - 1) >> 7, 0, CH - 1), (held - 1) & 127

    def lanes_packed(load, at, ys):
        acc = zero
        for y in ys:
            acc = jnp.where(lane == y, rolled(load(y), (y - at) & 127) if not isinstance(at, int) else pltpu.roll(load(y), (y - at) & 127, 1), acc)
        return acc

    def first_of(u, x, ys):
        return lanes_packed(lambda y: u[x + 1, y, 0], 0, ys)

    def last_of(u, x, ys):
        return lanes_packed(lambda y: u[x + 1, y, last_chunk], last_lane, ys)

    def fill_x(u, left_tile, right_tile, ys):
        for y in ys:
            from_left = jnp.broadcast_to(left_tile[:, y : y + 1], (8, 128))
            from_right = jnp.broadcast_to(right_tile[:, y : y + 1], (8, 128))
            turned = [pltpu.roll(u[1, y, c], 127, 1) for c in range(CH)]
            for c in range(CH):
                value = jnp.where(lane < 127, turned[c], turned[min(c + 1, CH - 1)])
                u[9, y, c] = jnp.where(lane + 128 * c == held - 1, from_right, value)
            turned = [pltpu.roll(u[8, y, c], 1, 1) for c in range(CH)]
            for c in range(CH):
                u[0, y, c] = jnp.where(lane > 0, turned[c], turned[c - 1] if c else from_left)

    def along_z(value):
        up = jnp.where(sub < 7, pltpu.roll(value, 7, 0), 0.0)
        down = jnp.where(sub > 0, pltpu.roll(value, 1, 0), 0.0)
        return up + down

    def sweep(u, first, ys, store):
        need = sorted({y + d for y in ys for d in (-1, 0, 1)} & set(range(8)))

        def body(x, carry):
            for c in range(CH):
                here = {y: u[x + 1, y, c] for y in need}
                here[-1] = yh[0, x, c] if 0 in ys else None
                here[8] = yh[1, x, c] if 7 in ys else None
                for y in ys:
                    total = u[x, y, c] + u[x + 2, y, c]
                    total = total + (here[y - 1] + here[y + 1]) + along_z(here[y])
                    if first:
                        scale = 1.0 / (6.0 + raw_c[x, y, pl.ds(c, 8, stride=CH), :])
                        inv[x, y, c] = scale
                    else:
                        scale = inv[x, y, c]
                    store(x, y, c, (raw_s[x, y, pl.ds(c, 8, stride=CH), :] + total) * scale)
            return carry

        lax.fori_loop(0, 8, body, 0)

    def store_u1(x, y, c, value):
        u1[x + 1, y, c] = value

    def store_wide(x, y, c, value):
        wide[x, y, c + 2] = value

    def ends(group):
        start, size = GROUPS[group]

        def body(x, carry):
            for p in range(start, start + size):
                y = ORDER[p]
                got = shifted(lambda k: wide[x, y, k + 2], held - HALF, range(2), 2, 10)
                for k in range(2):
                    t2s[p, x, k] = got[k]
                    h2s[p, x, k] = wide[x, y, k + 2]
            return carry

        lax.fori_loop(0, 8, body, 0)

    def halo(rx, side, exists, drift_prev):
        @pl.when(exists)
        def _():
            tile = cb3[side]
            other_prev = tile[0, 0] - rank * AVG
            other_next = tile[1, 0] - (rank + 1) * AVG
            begin = 512 + drift_prev - other_prev
            begin_next = 1024 + drift_prev - other_next

            def body(x, carry):
                load = lambda k: rx[side, x, k]
                own = shifted(load, begin, range(CH), 0, 8)
                later = shifted(load, begin_next, range(4, CH), 4, 12)
                for c in range(CH):
                    value = own[c]
                    if c >= 4:
                        value = jnp.where(lane + 128 * c + drift_prev >= AVG + other_next, later[c], value)
                    yh[side, x, c] = value
                return carry

            lax.fori_loop(0, 8, body, 0)

        @pl.when(jnp.logical_not(exists))
        def _():
            def body(x, carry):
                for c in range(CH):
                    yh[side, x, c] = zero
                return carry

            lax.fori_loop(0, 8, body, 0)

    def y_parts(group):
        return ((pl.ds(2, 4),), (pl.ds(1, 1), pl.ds(6, 1)), (pl.ds(0, 1), pl.ds(7, 1)))[group]

    results = []
    for group in range(3):
        results.append([
            pltpu.make_async_copy(
                flat.at[:, part], out.at[:, part], out_sem.at[group, i])
            for i, part in enumerate(y_parts(group))
        ])

    def finish(group, drift_prev, drift_next):
        for move in moves[group]:
            move.wait_recv()
        start, size = GROUPS[group]

        def body(x, carry):
            for p in range(start, start + size):
                y = ORDER[p]
                for k in range(2):
                    wide[x, y, k] = t2r[p, x, k]
                    wide[x, y, 14 + k] = h2r[p, x, k]
                load = lambda k: wide[x, y, k]
                own = shifted(load, HALF - drift_prev, range(8), 0, 4)
                later = shifted(load, 768 - drift_next, range(6, 8), 4, 8)
                for k in range(8):
                    value = own[k]
                    if k >= 6:
                        value = jnp.where(lane + 128 * k >= AVG + drift_next, later[k], value)
                    flat[x, y, pl.ds(k, 8, stride=8), :] = value
            return carry

        lax.fori_loop(0, 8, body, 0)
        for result in results[group]:
            result.start()

    for key in first_loads[:8]:
        loads[key].wait()
    lax.fori_loop(0, 8, convert, 0)
    cs[0] = jnp.full((8, 128), held, jnp.int32)
    cb1[zc] = jnp.full((8, 128), held, jnp.int32)
    plane_tails(u0, ts0)
    for key in first_loads[8:]:
        loads[key].wait()
    every = range(8)
    ps[0, 0] = first_of(u0, 0, every)
    ps[0, 1] = first_of(u0, 1, every)
    ps[1, 0] = last_of(u0, 7, every)
    ps[1, 1] = last_of(u0, 6, every)
    for k, raw in ((2, raw_s), (3, raw_c)):
        ps[0, k] = lanes_packed(lambda y: raw[0, y, pl.ds(0, 8, stride=CH), :], 0, every)

        def last_tile(y):
            tile = raw[7, y, pl.ds(0, 8, stride=CH), :]
            for c in range(1, CH):
                tile = jnp.where(last_chunk == c, raw[7, y, pl.ds(c, 8, stride=CH), :], tile)
            return tile

        ps[1, k] = lanes_packed(last_tile, last_lane, every)

    pl.semaphore_wait(barrier, len(peers))
    for m in packs + count_z + planes0:
        m.start()

    for key in other_loads:
        loads[key].wait()
    for m in packs:
        m.wait_recv()
    left0 = jnp.where(has_left, pr[0, 0], zero)
    right0 = jnp.where(has_right, pr[1, 0], zero)
    fill_x(u0, left0, right0, every)
    sweep(u0, True, range(1, 7), store_u1)

    def edge_u1(side, own, exists):
        u = pr[side, 0]
        along_y = jnp.where(lane < 7, pltpu.roll(u, 127, 1), 0.0) + jnp.where(lane > 0, pltpu.roll(u, 1, 1), 0.0)
        total = pr[side, 1] + own + along_y + along_z(u)
        return jnp.where(exists, (pr[side, 2] + total) / (6.0 + pr[side, 3]), zero)

    left1 = edge_u1(0, ps[0, 0], has_left)
    right1 = edge_u1(1, ps[1, 0], has_right)
    fill_x(u1, left1, right1, range(1, 7))

    for m in count_z:
        m.wait_recv()
    line = jnp.zeros((8, 128), jnp.int32)
    before = line
    for z in range(NZ):
        tile = cb1[z]
        line = line + tile
        before = before + jnp.where(z < zc, tile, 0)
    cs[1] = line
    cb2[xc] = line
    for m in count_x:
        m.start()

    sweep(u1, False, range(2, 6), store_wide)
    ends(0)
    for m in moves[0]:
        m.start()

    for m in count_x:
        m.wait_recv()
    for x in range(NX):
        before = before + jnp.where(x < xc, cb2[x], 0)
    cs[2] = jnp.where(sub == 0, before, before + held)
    for m in count_g:
        m.start()
    drift_prev = before[0, 0] - rank * AVG
    drift_next = drift_prev + held - AVG

    for m in planes0 + count_g:
        m.wait_recv()
    halo(rx0, 0, has_low, drift_prev)
    halo(rx0, 1, has_high, drift_prev)
    sweep(u0, True, (0, 7), store_u1)
    plane_tails(u1, ts1)
    ls[0] = first_of(u1, 0, (0, 7))
    ls[1] = last_of(u1, 7, (0, 7))
    for m in late_packs + planes1:
        m.start()

    sweep(u1, False, (1, 6), store_wide)
    ends(1)
    for m in moves[1]:
        m.start()
    finish(0, drift_prev, drift_next)

    for m in late_packs:
        m.wait_recv()
    fill_x(u1, jnp.where(has_left, lr[0], zero), jnp.where(has_right, lr[1], zero), (0, 7))
    for m in planes1:
        m.wait_recv()
    halo(rx1, 0, has_low, drift_prev)
    halo(rx1, 1, has_high, drift_prev)
    sweep(u1, False, (0, 7), store_wide)
    ends(2)
    for m in moves[2]:
        m.start()
    finish(1, drift_prev, drift_next)
    finish(2, drift_prev, drift_next)

    for m in packs + count_z + planes0 + count_x + count_g + late_packs + planes1:
        m.wait_send()
    for pair in moves:
        for m in pair:
            m.wait_send()
    for group in results:
        for result in group:
            result.wait()


N_MESSAGES = (NZ - 1) + (NX - 1) + 2 + 2 + 2 + 6 + 6 + 6


def local(state, coef, counts):
    f32, i32 = jnp.float32, jnp.int32
    vmem = pltpu.VMEM
    result = pl.pallas_call(
        kernel,
        out_shape=jax.ShapeDtypeStruct((8, 8, 64, 128), f32),
        in_specs=[
            pl.BlockSpec(memory_space=pltpu.SMEM),
            pl.BlockSpec(memory_space=pl.ANY),
            pl.BlockSpec(memory_space=pl.ANY),
        ],
        out_specs=pl.BlockSpec(memory_space=pl.ANY),
        scratch_shapes=[
            vmem((8, 8, 96, 128), f32), vmem((8, 8, 96, 128), f32), vmem((8, 8, 96, 128), f32),
            vmem((10, 8, CH, 8, 128), f32), vmem((10, 8, CH, 8, 128), f32), vmem((8, 8, CH, 8, 128), f32),
            vmem((2, 8, CH, 8, 128), f32),
            vmem((2, 8, 25, 8, 128), f32), vmem((2, 8, 25, 8, 128), f32),
            vmem((2, 8, 4, 8, 128), f32), vmem((2, 8, 4, 8, 128), f32),
            vmem((2, 4, 8, 128), f32), vmem((2, 4, 8, 128), f32),
            vmem((2, 8, 128), f32), vmem((2, 8, 128), f32),
            vmem((8, 8, 2, 8, 128), f32), vmem((8, 8, 2, 8, 128), f32),
            vmem((8, 8, 2, 8, 128), f32), vmem((8, 8, 2, 8, 128), f32),
            vmem((8, 8, 17, 8, 128), f32), vmem((8, 8, 64, 128), f32),
            vmem((NZ, 8, 128), i32), vmem((NX, 8, 128), i32), vmem((2, 8, 128), i32), vmem((3, 8, 128), i32),
            pltpu.SemaphoreType.DMA((3, 8)), pltpu.SemaphoreType.DMA((3, 2)),
            pltpu.SemaphoreType.DMA((N_MESSAGES,)), pltpu.SemaphoreType.DMA((N_MESSAGES,)),
        ],
        compiler_params=pltpu.CompilerParams(
            collective_id=0, has_side_effects=True, vmem_limit_bytes=60 * 1024 * 1024),
    )(counts, state.reshape(2, 8, 8, 96, 128), coef.reshape(8, 8, 96, 128))
    return result.reshape(512, 1, AVG)


def solution(mesh):
    placed = (P(None, None, "grp", "curve"), P(None, "grp", "curve"), P("grp", "curve"))
    return jax.shard_map(
        local, mesh=mesh, in_specs=placed, out_specs=P(None, "grp", "curve"), check_vma=False
    )
```

```python
import jax
import jax.numpy as jnp
from jax import lax
from jax.experimental import pallas as pl
from jax.experimental.pallas import tpu as pltpu
from jax.sharding import PartitionSpec as P

AVG = 1024
HALF = 256
CAP = 1536
N_CURVE = 32
N_GRP = 8
CH = CAP // 128
MESH = pl.DeviceIdType.MESH
ORDER = (2, 3, 4, 5, 1, 6, 0, 7)
GROUPS = ((0, 4), (4, 2), (6, 2))


class Message:
    def __init__(self, make, sends, receives):
        self.make, self.sends, self.receives = make, sends, receives

    def start(self):
        pl.when(self.sends)(lambda: self.make().start())

    def wait_recv(self):
        pl.when(self.receives)(lambda: self.make().wait_recv())

    def wait_send(self):
        pl.when(self.sends)(lambda: self.make().wait_send())


def kernel(
    counts, state, coef, out,
    raw_u, raw_s, raw_c, u0, u1, inv, yh, rx0, rx1, ts0, ts1, ps, pr, ls, lr,
    t2s, t2r, h2s, h2r, wide, cb, cb3, cs, cs3,
    in_sem, send_sem, recv_sem,
):
    rank, grp = lax.axis_index("curve"), lax.axis_index("grp")
    has_left, has_right = rank > 0, rank < N_CURVE - 1
    has_low, has_high = grp > 0, grp < N_GRP - 1
    left, right = (rank + N_CURVE - 1) % N_CURVE, (rank + 1) % N_CURVE
    low, high = (grp + N_GRP - 1) % N_GRP, (grp + 1) % N_GRP

    barrier = pltpu.get_barrier_semaphore()
    peers = [(r, g) for g in (low, high) for r in (left, rank, right)]
    peers += [((rank + k) % N_CURVE, grp) for k in range(1, N_CURVE)]
    for peer in peers:
        pl.semaphore_signal(barrier, inc=1, device_id=peer, device_id_type=MESH)

    loads = {}
    for kind, src, dst in ((0, state.at[0], raw_u), (1, state.at[1], raw_s), (2, coef, raw_c)):
        for x in range(8):
            loads[kind, x] = pltpu.make_async_copy(src.at[x], dst.at[x], in_sem.at[kind, x])
    first_loads = [(0, x) for x in range(8)] + [(1, 0), (1, 7), (2, 0), (2, 7)]
    other_loads = [(kind, x) for x in range(1, 7) for kind in (1, 2)]
    for key in first_loads:
        loads[key].start()

    lane = lax.broadcasted_iota(jnp.int32, (8, 128), 1)
    sub = lax.broadcasted_iota(jnp.int32, (8, 128), 0)
    zero = jnp.zeros((8, 128), jnp.float32)
    held = counts[0, 0]

    index = [0]

    def message(src, dst, device, sends, receives):
        at = index[0]
        index[0] += 1

        def make():
            return pltpu.make_async_remote_copy(
                src_ref=src(), dst_ref=dst(), send_sem=send_sem.at[at], recv_sem=recv_sem.at[at],
                device_id=device, device_id_type=MESH,
            )

        return Message(make, sends, receives)

    yes = rank >= 0
    count_all = [
        message(lambda: cs, lambda: cb.at[rank], ((rank + k) % N_CURVE, grp), yes, yes)
        for k in range(1, N_CURVE)
    ]
    count_g = [
        message(lambda: cs3, lambda: cb3.at[1], (rank, low), has_low, has_high),
        message(lambda: cs3, lambda: cb3.at[0], (rank, high), has_high, has_low),
    ]
    packs = [
        message(lambda: ps.at[0], lambda: pr.at[1], (left, grp), has_left, has_right),
        message(lambda: ps.at[1], lambda: pr.at[0], (right, grp), has_right, has_left),
    ]
    late_packs = [
        message(lambda: ls.at[0], lambda: lr.at[1], (left, grp), has_left, has_right),
        message(lambda: ls.at[1], lambda: lr.at[0], (right, grp), has_right, has_left),
    ]

    def planes_out(u, ts, rx):
        tails, heads, mids = [], [], []
        for d, y, other, sends, receives in (
            (0, 0, low, has_low, has_high), (1, 7, high, has_high, has_low),
        ):
            tails.append(message(
                lambda d=d: ts.at[d], lambda d=d: rx.at[1 - d, :, pl.ds(0, 4)], (right, other),
                jnp.logical_and(sends, has_right), jnp.logical_and(receives, has_left)))
            heads.append(message(
                lambda y=y: u.at[pl.ds(1, 8), y, pl.ds(0, 4)],
                lambda d=d: rx.at[1 - d, :, pl.ds(16, 4)], (left, other),
                jnp.logical_and(sends, has_left), jnp.logical_and(receives, has_right)))
            mids.append(message(
                lambda y=y: u.at[pl.ds(1, 8), y], lambda d=d: rx.at[1 - d, :, pl.ds(4, 12)],
                (rank, other), sends, receives))
        return tails + heads + mids

    planes0 = planes_out(u0, ts0, rx0)
    planes1 = planes_out(u1, ts1, rx1)
    moves = []
    for start, size in GROUPS:
        part = pl.ds(start, size)
        moves.append([
            message(lambda part=part: t2s.at[part], lambda part=part: t2r.at[part], (right, grp),
                    has_right, has_left),
            message(lambda part=part: h2s.at[part], lambda part=part: h2r.at[part], (left, grp),
                    has_left, has_right),
        ])

    def loop(start, stop, body, unroll=1):
        if unroll == stop - start:
            for x in range(start, stop):
                body(x)
            return

        def step(i, carry):
            for k in range(unroll):
                body(start + i * unroll + k)
            return carry

        lax.fori_loop(0, (stop - start) // unroll, step, 0)

    def rolled(value, turn):
        return pltpu.roll(value, turn, 1)

    def shifted(load, start, chunks, lowest, highest):
        first, offset = jnp.clip(start >> 7, lowest, highest), start & 127
        turn = (128 - offset) & 127
        turned = {}
        for k in sorted(set(chunks) | {k + 1 for k in chunks}):
            turned[k] = rolled(load(first + k), turn)
        keep = lane < 128 - offset
        return {k: jnp.where(keep, turned[k], turned[k + 1]) for k in chunks}

    def convert(x):
        for y in range(8):
            for c in range(CH):
                u0[x + 1, y, c] = raw_u[x, y, pl.ds(c, 8, stride=CH), :]

    def plane_tails(u, ts):
        def body(x):
            for d, y in ((0, 0), (1, 7)):
                got = shifted(
                    lambda k: u[x + 1, y, jnp.minimum(k, CH - 1)], held - 512, range(4), 0, 8)
                for k in range(4):
                    ts[d, x, k] = got[k]

        loop(0, 8, body, 8)

    last_chunk, last_lane = jnp.clip((held - 1) >> 7, 0, CH - 1), (held - 1) & 127

    def lanes_packed(load, at, ys):
        acc = zero
        for y in ys:
            acc = jnp.where(lane == y, rolled(load(y), (y - at) & 127) if not isinstance(at, int) else pltpu.roll(load(y), (y - at) & 127, 1), acc)
        return acc

    def first_of(u, x, ys):
        return lanes_packed(lambda y: u[x + 1, y, 0], 0, ys)

    def last_of(u, x, ys):
        return lanes_packed(lambda y: u[x + 1, y, last_chunk], last_lane, ys)

    def fill_x(u, left_tile, right_tile, ys):
        for y in ys:
            from_left = jnp.broadcast_to(left_tile[:, y : y + 1], (8, 128))
            from_right = jnp.broadcast_to(right_tile[:, y : y + 1], (8, 128))
            turned = [pltpu.roll(u[1, y, c], 127, 1) for c in range(CH)]
            for c in range(CH):
                value = jnp.where(lane < 127, turned[c], turned[min(c + 1, CH - 1)])
                u[9, y, c] = jnp.where(lane + 128 * c == held - 1, from_right, value)
            turned = [pltpu.roll(u[8, y, c], 1, 1) for c in range(CH)]
            for c in range(CH):
                u[0, y, c] = jnp.where(lane > 0, turned[c], turned[c - 1] if c else from_left)

    def along_z(value):
        up = jnp.where(sub < 7, pltpu.roll(value, 7, 0), 0.0)
        down = jnp.where(sub > 0, pltpu.roll(value, 1, 0), 0.0)
        return up + down

    def sweep(u, first, ys, store, xs=(0, 8, 1)):
        need = sorted({y + d for y in ys for d in (-1, 0, 1)} & set(range(8)))

        def body(x):
            for c in range(CH):
                here = {y: u[x + 1, y, c] for y in need}
                here[-1] = yh[0, x, c] if 0 in ys else None
                here[8] = yh[1, x, c] if 7 in ys else None
                for y in ys:
                    total = u[x, y, c] + u[x + 2, y, c]
                    total = total + (here[y - 1] + here[y + 1]) + along_z(here[y])
                    if first:
                        scale = 1.0 / (6.0 + raw_c[x, y, pl.ds(c, 8, stride=CH), :])
                        inv[x, y, c] = scale
                    else:
                        scale = inv[x, y, c]
                    store(x, y, c, (raw_s[x, y, pl.ds(c, 8, stride=CH), :] + total) * scale)

        loop(xs[0], xs[1], body, xs[2])

    def store_u1(x, y, c, value):
        u1[x + 1, y, c] = value

    def store_wide(x, y, c, value):
        wide[x, y, c + 2] = value

    def ends(group):
        start, size = GROUPS[group]

        def body(x):
            for p in range(start, start + size):
                y = ORDER[p]
                got = shifted(lambda k: wide[x, y, k + 2], held - HALF, range(2), 2, 10)
                for k in range(2):
                    t2s[p, x, k] = got[k]
                    h2s[p, x, k] = wide[x, y, k + 2]

        loop(0, 8, body, 8)

    def halos(rx, drift_prev):
        starts = []
        for side in range(2):
            tile = cb3[side]
            other_prev = tile[0, 0] - rank * AVG
            other_next = tile[1, 0] - (rank + 1) * AVG
            starts.append((AVG // 2 + drift_prev - other_prev, AVG + drift_prev - other_next))

        def body(x):
            for side, exists in ((0, has_low), (1, has_high)):
                load = lambda k: rx[side, x, k]
                begin, begin_next = starts[side]
                own = shifted(load, begin, range(CH), 0, 8)
                later = shifted(load, begin_next, range(4, CH), 4, 12)
                for c in range(CH):
                    value = own[c]
                    if c >= 4:
                        value = jnp.where(lane + 128 * c >= 2 * AVG - begin_next, later[c], value)
                    yh[side, x, c] = jnp.where(exists, value, zero)

        loop(0, 8, body, 4)

    def finish(group, drift_prev, drift_next):
        for move in moves[group]:
            move.wait_recv()
        start, size = GROUPS[group]

        def body(x):
            for p in range(start, start + size):
                y = ORDER[p]
                for k in range(2):
                    wide[x, y, k] = t2r[p, x, k]
                    wide[x, y, 14 + k] = h2r[p, x, k]
                load = lambda k: wide[x, y, k]
                own = shifted(load, HALF - drift_prev, range(8), 0, 4)
                later = shifted(load, 768 - drift_next, range(6, 8), 4, 8)
                for k in range(8):
                    value = own[k]
                    if k >= 6:
                        value = jnp.where(lane + 128 * k >= AVG + drift_next, later[k], value)
                    out[x, y, pl.ds(k, 8, stride=8), :] = value

        loop(0, 8, body, 8 // size)

    for key in first_loads[:8]:
        loads[key].wait()
    for key in other_loads:
        loads[key].start()
    loop(0, 8, convert)
    cs[...] = jnp.full((1, 128), held, jnp.int32)
    plane_tails(u0, ts0)
    for key in first_loads[8:]:
        loads[key].wait()
    every = range(8)
    ps[0, 0] = first_of(u0, 0, every)
    ps[0, 1] = first_of(u0, 1, every)
    ps[1, 0] = last_of(u0, 7, every)
    ps[1, 1] = last_of(u0, 6, every)
    for k, raw in ((2, raw_s), (3, raw_c)):
        ps[0, k] = lanes_packed(lambda y: raw[0, y, pl.ds(0, 8, stride=CH), :], 0, every)

        def last_tile(y):
            tile = raw[7, y, pl.ds(0, 8, stride=CH), :]
            for c in range(1, CH):
                tile = jnp.where(last_chunk == c, raw[7, y, pl.ds(c, 8, stride=CH), :], tile)
            return tile

        ps[1, k] = lanes_packed(last_tile, last_lane, every)

    pl.semaphore_wait(barrier, len(peers))
    for m in packs + count_all + planes0:
        m.start()

    for key in other_loads:
        loads[key].wait()
    sweep(u0, True, range(1, 7), store_u1, (1, 7, 1))
    for m in packs:
        m.wait_recv()
    left0 = jnp.where(has_left, pr[0, 0], zero)
    right0 = jnp.where(has_right, pr[1, 0], zero)
    fill_x(u0, left0, right0, every)
    sweep(u0, True, range(1, 7), store_u1, (0, 1, 1))
    sweep(u0, True, range(1, 7), store_u1, (7, 8, 1))

    def edge_u1(side, own, exists):
        u = pr[side, 0]
        along_y = jnp.where(lane < 7, pltpu.roll(u, 127, 1), 0.0) + jnp.where(lane > 0, pltpu.roll(u, 1, 1), 0.0)
        total = pr[side, 1] + own + along_y + along_z(u)
        return jnp.where(exists, (pr[side, 2] + total) / (6.0 + pr[side, 3]), zero)

    left1 = edge_u1(0, ps[0, 0], has_left)
    right1 = edge_u1(1, ps[1, 0], has_right)
    fill_x(u1, left1, right1, range(1, 7))
    sweep(u1, False, range(2, 6), store_wide)
    ends(0)
    for m in moves[0]:
        m.start()

    for m in count_all:
        m.wait_recv()
    before = jnp.zeros((1, 128), jnp.int32)
    for r in range(N_CURVE - 1):
        before = before + jnp.where(r < rank, cb[r], 0)
    drift_prev = before[0, 0] - rank * AVG
    drift_next = drift_prev + held - AVG
    cs3[...] = jnp.where(sub == 0, before, before + held)
    for m in count_g:
        m.start()

    for m in planes0 + count_g:
        m.wait_recv()
    halos(rx0, drift_prev)
    sweep(u0, True, (0, 7), store_u1)
    plane_tails(u1, ts1)
    ls[0] = first_of(u1, 0, (0, 7))
    ls[1] = last_of(u1, 7, (0, 7))
    for m in late_packs + planes1:
        m.start()

    sweep(u1, False, (1, 6), store_wide)
    ends(1)
    for m in moves[1]:
        m.start()
    finish(0, drift_prev, drift_next)

    for m in late_packs:
        m.wait_recv()
    fill_x(u1, jnp.where(has_left, lr[0], zero), jnp.where(has_right, lr[1], zero), (0, 7))
    for m in planes1:
        m.wait_recv()
    halos(rx1, drift_prev)
    sweep(u1, False, (0, 7), store_wide)
    ends(2)
    for m in moves[2]:
        m.start()
    finish(1, drift_prev, drift_next)
    finish(2, drift_prev, drift_next)

    for m in packs + count_all + planes0 + count_g + late_packs + planes1:
        m.wait_send()
    for pair in moves:
        for m in pair:
            m.wait_send()


N_MESSAGES = (N_CURVE - 1) + 2 + 2 + 2 + 6 + 6 + 6


def local(state, coef, counts):
    f32, i32 = jnp.float32, jnp.int32
    vmem = pltpu.VMEM
    result = pl.pallas_call(
        kernel,
        out_shape=vmem((8, 8, 64, 128), f32),
        in_specs=[
            pl.BlockSpec(memory_space=pltpu.SMEM),
            pl.BlockSpec(memory_space=pl.ANY),
            pl.BlockSpec(memory_space=pl.ANY),
        ],
        out_specs=pl.BlockSpec(memory_space=vmem),
        scratch_shapes=[
            vmem((8, 8, 96, 128), f32), vmem((8, 8, 96, 128), f32), vmem((8, 8, 96, 128), f32),
            vmem((10, 8, CH, 8, 128), f32), vmem((10, 8, CH, 8, 128), f32), vmem((8, 8, CH, 8, 128), f32),
            vmem((2, 8, CH, 8, 128), f32),
            vmem((2, 8, 25, 8, 128), f32), vmem((2, 8, 25, 8, 128), f32),
            vmem((2, 8, 4, 8, 128), f32), vmem((2, 8, 4, 8, 128), f32),
            vmem((2, 4, 8, 128), f32), vmem((2, 4, 8, 128), f32),
            vmem((2, 8, 128), f32), vmem((2, 8, 128), f32),
            vmem((8, 8, 2, 8, 128), f32), vmem((8, 8, 2, 8, 128), f32),
            vmem((8, 8, 2, 8, 128), f32), vmem((8, 8, 2, 8, 128), f32),
            vmem((8, 8, 17, 8, 128), f32),
            vmem((N_CURVE, 1, 128), i32), vmem((2, 8, 128), i32), vmem((1, 128), i32), vmem((8, 128), i32),
            pltpu.SemaphoreType.DMA((3, 8)),
            pltpu.SemaphoreType.DMA((N_MESSAGES,)), pltpu.SemaphoreType.DMA((N_MESSAGES,)),
        ],
        compiler_params=pltpu.CompilerParams(
            collective_id=0, has_side_effects=True, vmem_limit_bytes=60 * 1024 * 1024),
    )(counts, state.reshape(2, 8, 8, 96, 128), coef.reshape(8, 8, 96, 128))
    return result.reshape(512, 1, AVG)


def solution(mesh):
    placed = (P(None, None, "grp", "curve"), P(None, "grp", "curve"), P("grp", "curve"))
    return jax.shard_map(
        local, mesh=mesh, in_specs=placed, out_specs=P(None, "grp", "curve"), check_vma=False
    )
```

```python
import jax
import jax.numpy as jnp
from jax import lax
from jax.experimental import pallas as pl
from jax.experimental.pallas import tpu as pltpu
from jax.sharding import PartitionSpec as P

AVG = 1024
HALF = 256
CAP = 1536
NX, NZ = 4, 8
N_CURVE = NX * NZ
N_GRP = 8
CH = CAP // 128
MESH = pl.DeviceIdType.MESH
ORDER = (2, 3, 4, 5, 1, 6, 0, 7)
INNER, EDGE_LOW, EDGE_HIGH, NEXT, LAST_LOW, LAST_HIGH = PARTS = (
    (0, 4, 2, 4), (0, 4, 0, 2), (0, 4, 6, 2), (4, 2, 0, 8), (6, 1, 0, 8), (7, 1, 0, 8),
)


class Message:
    def __init__(self, make, sends, receives):
        self.make, self.sends, self.receives = make, sends, receives

    def start(self):
        pl.when(self.sends)(lambda: self.make().start())

    def wait_recv(self):
        pl.when(self.receives)(lambda: self.make().wait_recv())

    def wait_send(self):
        pl.when(self.sends)(lambda: self.make().wait_send())


def kernel(
    counts, state, coef, out,
    raw_u, raw_s, raw_c, u0, u1, inv, yh, rx0, rx1, ts0, ts1, ps, pr, ls, lr,
    t2s, t2r, h2s, h2r, wide, cbx, cbz, cb3, cs, cs3,

    in_sem, send_sem, recv_sem,
):
    rank, grp = lax.axis_index("curve"), lax.axis_index("grp")
    xc, zc = rank // NZ, rank % NZ
    has_left, has_right = rank > 0, rank < N_CURVE - 1
    has_low, has_high = grp > 0, grp < N_GRP - 1
    left, right = (rank + N_CURVE - 1) % N_CURVE, (rank + 1) % N_CURVE
    low, high = (grp + N_GRP - 1) % N_GRP, (grp + 1) % N_GRP

    barrier = pltpu.get_barrier_semaphore()
    peers = [(r, g) for g in (low, high) for r in (left, rank, right)]
    peers += [(left, grp), (right, grp)]
    peers += [(((xc + k) % NX) * NZ + zc, grp) for k in range(1, NX)]
    peers += [(xc * NZ + (zc + k) % NZ, grp) for k in range(1, NZ)]
    loads = {}
    for kind, src, dst in ((0, state.at[0], raw_u), (1, state.at[1], raw_s), (2, coef, raw_c)):
        for x in range(8):
            loads[kind, x] = pltpu.make_async_copy(src.at[x], dst.at[x], in_sem.at[kind, x])
    first_loads = [(0, x) for x in range(8)] + [(1, 0), (1, 7), (2, 0), (2, 7)]
    other_loads = [(kind, x) for x in range(1, 7) for kind in (1, 2)]
    for key in first_loads:
        loads[key].start()
    for peer in peers:
        pl.semaphore_signal(barrier, inc=1, device_id=peer, device_id_type=MESH)

    lane = lax.broadcasted_iota(jnp.int32, (8, 128), 1)
    sub = lax.broadcasted_iota(jnp.int32, (8, 128), 0)
    zero = jnp.zeros((8, 128), jnp.float32)
    held = counts[0, 0]

    index = [0]

    def message(src, dst, device, sends, receives):
        at = index[0]
        index[0] += 1

        def make():
            return pltpu.make_async_remote_copy(
                src_ref=src(), dst_ref=dst(), send_sem=send_sem.at[at], recv_sem=recv_sem.at[at],
                device_id=device, device_id_type=MESH,
            )

        return Message(make, sends, receives)

    yes = rank >= 0
    count_x = [
        message(lambda: cs, lambda: cbx.at[xc], (((xc + k) % NX) * NZ + zc, grp), yes, yes)
        for k in range(1, NX)
    ]
    count_z = [
        message(lambda: cbx, lambda: cbz.at[zc], (xc * NZ + (zc + k) % NZ, grp), yes, yes)
        for k in range(1, NZ)
    ]
    count_g = [
        message(lambda: cs3, lambda: cb3.at[1], (rank, low), has_low, has_high),
        message(lambda: cs3, lambda: cb3.at[0], (rank, high), has_high, has_low),
    ]
    packs = [
        message(lambda: ps.at[0], lambda: pr.at[1], (left, grp), has_left, has_right),
        message(lambda: ps.at[1], lambda: pr.at[0], (right, grp), has_right, has_left),
    ]
    late_packs = [
        message(lambda: ls.at[0], lambda: lr.at[1], (left, grp), has_left, has_right),
        message(lambda: ls.at[1], lambda: lr.at[0], (right, grp), has_right, has_left),
    ]

    def planes_out(u, ts, rx):
        tails, heads, mids = [], [], []
        for d, y, other, sends, receives in (
            (0, 0, low, has_low, has_high), (1, 7, high, has_high, has_low),
        ):
            tails.append(message(
                lambda d=d: ts.at[d], lambda d=d: rx.at[1 - d, :, pl.ds(0, 4)], (right, other),
                jnp.logical_and(sends, has_right), jnp.logical_and(receives, has_left)))
            heads.append(message(
                lambda y=y: u.at[pl.ds(1, 8), y, pl.ds(0, 4)],
                lambda d=d: rx.at[1 - d, :, pl.ds(16, 4)], (left, other),
                jnp.logical_and(sends, has_left), jnp.logical_and(receives, has_right)))
            mids.append(message(
                lambda y=y: u.at[pl.ds(1, 8), y], lambda d=d: rx.at[1 - d, :, pl.ds(4, 12)],
                (rank, other), sends, receives))
        return [tails[0], heads[0]], mids, [tails[1], heads[1]]

    planes0_low, planes0_mid, planes0_high = planes_out(u0, ts0, rx0)
    planes0 = planes0_low + planes0_mid + planes0_high
    planes1_low, planes1_mid, planes1_high = planes_out(u1, ts1, rx1)
    planes1 = planes1_low + planes1_high + planes1_mid
    moves = {}
    for part in PARTS:
        at = (pl.ds(part[0], part[1]), pl.ds(part[2], part[3]))
        moves[part] = [
            message(lambda at=at: t2s.at[at], lambda at=at: t2r.at[at], (right, grp), has_right, has_left),
            message(lambda at=at: h2s.at[at], lambda at=at: h2r.at[at], (left, grp), has_left, has_right),
        ]

    def loop(start, stop, body, unroll=1):
        if unroll == stop - start:
            for x in range(start, stop):
                body(x)
            return

        def step(i, carry):
            for k in range(unroll):
                body(start + i * unroll + k)
            return carry

        lax.fori_loop(0, (stop - start) // unroll, step, 0)

    def rolled(value, turn):
        return pltpu.roll(value, turn, 1)

    def shifted(load, start, chunks, lowest, highest):
        first, offset = jnp.clip(start >> 7, lowest, highest), start & 127
        turn = (128 - offset) & 127
        turned = {}
        for k in sorted(set(chunks) | {k + 1 for k in chunks}):
            turned[k] = rolled(load(first + k), turn)
        keep = lane < 128 - offset
        return {k: jnp.where(keep, turned[k], turned[k + 1]) for k in chunks}

    def convert(x):
        for y in range(8):
            for c in range(CH):
                u0[x + 1, y, c] = raw_u[x, y, pl.ds(c, 8, stride=CH), :]

    def plane_tails(u, ts):
        def body(x):
            for d, y in ((0, 0), (1, 7)):
                got = shifted(
                    lambda k: u[x + 1, y, jnp.minimum(k, CH - 1)], held - 512, range(4), 0, 8)
                for k in range(4):
                    ts[d, x, k] = got[k]

        loop(0, 8, body, 8)

    last_chunk, last_lane = jnp.clip((held - 1) >> 7, 0, CH - 1), (held - 1) & 127

    def lanes_packed(load, at, ys):
        acc = zero
        for y in ys:
            acc = jnp.where(lane == y, rolled(load(y), (y - at) & 127) if not isinstance(at, int) else pltpu.roll(load(y), (y - at) & 127, 1), acc)
        return acc

    def first_of(u, x, ys):
        return lanes_packed(lambda y: u[x + 1, y, 0], 0, ys)

    def last_of(u, x, ys):
        return lanes_packed(lambda y: u[x + 1, y, last_chunk], last_lane, ys)

    def fill_x(u, left_tile, right_tile, ys):
        for y in ys:
            from_left = jnp.broadcast_to(left_tile[:, y : y + 1], (8, 128))
            from_right = jnp.broadcast_to(right_tile[:, y : y + 1], (8, 128))
            turned = [pltpu.roll(u[1, y, c], 127, 1) for c in range(CH)]
            for c in range(CH):
                value = jnp.where(lane < 127, turned[c], turned[min(c + 1, CH - 1)])
                u[9, y, c] = jnp.where(lane + 128 * c == held - 1, from_right, value)
            turned = [pltpu.roll(u[8, y, c], 1, 1) for c in range(CH)]
            for c in range(CH):
                u[0, y, c] = jnp.where(lane > 0, turned[c], turned[c - 1] if c else from_left)

    def along_z(value):
        up = jnp.where(sub < 7, pltpu.roll(value, 7, 0), 0.0)
        down = jnp.where(sub > 0, pltpu.roll(value, 1, 0), 0.0)
        return up + down

    def sweep(u, first, ys, store, xs=(0, 8, 1)):
        need = sorted({y + d for y in ys for d in (-1, 0, 1)} & set(range(8)))

        def body(x):
            for c in range(CH):
                here = {y: u[x + 1, y, c] for y in need}
                here[-1] = yh[0, x, c] if 0 in ys else None
                here[8] = yh[1, x, c] if 7 in ys else None
                for y in ys:
                    total = u[x, y, c] + u[x + 2, y, c]
                    total = total + (here[y - 1] + here[y + 1]) + along_z(here[y])
                    if first:
                        scale = 1.0 / (6.0 + raw_c[x, y, pl.ds(c, 8, stride=CH), :])
                        inv[x, y, c] = scale
                    else:
                        scale = inv[x, y, c]
                    store(x, y, c, (raw_s[x, y, pl.ds(c, 8, stride=CH), :] + total) * scale)

        loop(xs[0], xs[1], body, xs[2])

    def store_u1(x, y, c, value):
        u1[x + 1, y, c] = value

    def store_wide(x, y, c, value):
        wide[x, y, c + 2] = value

    def move(part):
        start, size, x_start, x_size = part

        def body(x):
            for p in range(start, start + size):
                y = ORDER[p]
                got = shifted(lambda k: wide[x, y, k + 2], held - HALF, range(2), 2, 10)
                for k in range(2):
                    t2s[p, x, k] = got[k]
                    h2s[p, x, k] = wide[x, y, k + 2]

        loop(x_start, x_start + x_size, body, x_size)

    def halos(rx, drift_prev):
        starts = []
        for side in range(2):
            tile = cb3[side]
            other_prev = tile[0, 0] - rank * AVG
            other_next = tile[1, 0] - (rank + 1) * AVG
            starts.append((AVG // 2 + drift_prev - other_prev, AVG + drift_prev - other_next))

        def body(x):
            for side, exists in ((0, has_low), (1, has_high)):
                load = lambda k: rx[side, x, k]
                begin, begin_next = starts[side]
                own = shifted(load, begin, range(CH), 0, 8)
                later = shifted(load, begin_next, range(4, CH), 4, 12)
                for c in range(CH):
                    value = own[c]
                    if c >= 4:
                        value = jnp.where(lane + 128 * c >= 2 * AVG - begin_next, later[c], value)
                    yh[side, x, c] = jnp.where(exists, value, zero)

        loop(0, 8, body, 4)

    def finish(part, drift_prev, drift_next):
        for m in moves[part]:
            m.wait_recv()
        start, size, x_start, x_size = part

        def body(x):
            for p in range(start, start + size):
                y = ORDER[p]
                for k in range(2):
                    wide[x, y, k] = t2r[p, x, k]
                    wide[x, y, 14 + k] = h2r[p, x, k]
                load = lambda k: wide[x, y, k]
                own = shifted(load, HALF - drift_prev, range(8), 0, 4)
                later = shifted(load, 768 - drift_next, range(6, 8), 4, 8)
                for k in range(8):
                    value = own[k]
                    if k >= 6:
                        value = jnp.where(lane + 128 * k >= AVG + drift_next, later[k], value)
                    out[x, y, pl.ds(k, 8, stride=8), :] = value

        loop(x_start, x_start + x_size, body, min(x_size, 8 // size))

    for key in first_loads[:8]:
        loads[key].wait()
    for key in other_loads:
        loads[key].start()
    loop(0, 8, convert)
    cs[...] = jnp.full((1, 128), held, jnp.int32)
    cbx[xc] = jnp.full((1, 128), held, jnp.int32)
    plane_tails(u0, ts0)
    for key in first_loads[8:]:
        loads[key].wait()
    every = range(8)
    ps[0, 0] = first_of(u0, 0, every)
    ps[0, 1] = first_of(u0, 1, every)
    ps[1, 0] = last_of(u0, 7, every)
    ps[1, 1] = last_of(u0, 6, every)
    for k, raw in ((2, raw_s), (3, raw_c)):
        ps[0, k] = lanes_packed(lambda y: raw[0, y, pl.ds(0, 8, stride=CH), :], 0, every)

        def last_tile(y):
            tile = raw[7, y, pl.ds(0, 8, stride=CH), :]
            for c in range(1, CH):
                tile = jnp.where(last_chunk == c, raw[7, y, pl.ds(c, 8, stride=CH), :], tile)
            return tile

        ps[1, k] = lanes_packed(last_tile, last_lane, every)

    pl.semaphore_wait(barrier, len(peers))
    for m in packs + count_x + planes0_low + planes0_mid:
        m.start()

    for key in other_loads:
        loads[key].wait()
    sweep(u0, True, range(1, 7), store_u1, (1, 7, 1))
    sweep(u1, False, range(2, 6), store_wide, (2, 6, 1))
    move(INNER)
    for m in count_x:
        m.wait_recv()
    for m in count_z + planes0_high + moves[INNER]:
        m.start()
    for m in packs:
        m.wait_recv()
    left0 = jnp.where(has_left, pr[0, 0], zero)
    right0 = jnp.where(has_right, pr[1, 0], zero)
    fill_x(u0, left0, right0, every)
    sweep(u0, True, range(1, 7), store_u1, (0, 1, 1))
    sweep(u0, True, range(1, 7), store_u1, (7, 8, 1))

    def edge_u1(side, own, exists):
        u = pr[side, 0]
        along_y = jnp.where(lane < 7, pltpu.roll(u, 127, 1), 0.0) + jnp.where(lane > 0, pltpu.roll(u, 1, 1), 0.0)
        total = pr[side, 1] + own + along_y + along_z(u)
        return jnp.where(exists, (pr[side, 2] + total) / (6.0 + pr[side, 3]), zero)

    left1 = edge_u1(0, ps[0, 0], has_left)
    right1 = edge_u1(1, ps[1, 0], has_right)
    fill_x(u1, left1, right1, range(1, 7))
    sweep(u1, False, range(2, 6), store_wide, (0, 2, 1))
    move(EDGE_LOW)
    for m in moves[EDGE_LOW]:
        m.start()
    sweep(u1, False, range(2, 6), store_wide, (6, 8, 1))
    move(EDGE_HIGH)

    for m in count_z:
        m.wait_recv()
    before = jnp.zeros((1, 128), jnp.int32)
    for x in range(NX):
        for z in range(NZ):
            row = jnp.where(z == zc, cbx[x], cbz[z, x])
            before = before + jnp.where(x * NZ + z < rank, row, 0)
    drift_prev = before[0, 0] - rank * AVG
    drift_next = drift_prev + held - AVG
    cs3[...] = jnp.where(sub == 0, before, before + held)
    for m in count_g:
        m.start()

    for m in planes0 + count_g:
        m.wait_recv()
    halos(rx0, drift_prev)
    sweep(u0, True, (0, 7), store_u1)
    plane_tails(u1, ts1)
    ls[0] = first_of(u1, 0, (0, 7))
    ls[1] = last_of(u1, 7, (0, 7))
    for m in late_packs + planes1 + moves[EDGE_HIGH]:
        m.start()

    sweep(u1, False, (1, 6), store_wide)
    move(NEXT)
    for m in moves[NEXT]:
        m.start()
    finish(INNER, drift_prev, drift_next)
    finish(EDGE_LOW, drift_prev, drift_next)

    for m in late_packs:
        m.wait_recv()
    fill_x(u1, jnp.where(has_left, lr[0], zero), jnp.where(has_right, lr[1], zero), (0, 7))
    for m in planes1:
        m.wait_recv()
    halos(rx1, drift_prev)
    sweep(u1, False, (0, 7), store_wide)
    move(LAST_LOW)
    move(LAST_HIGH)
    for m in moves[LAST_LOW] + moves[LAST_HIGH]:
        m.start()
    for part in (EDGE_HIGH, NEXT, LAST_LOW, LAST_HIGH):
        finish(part, drift_prev, drift_next)

    for m in packs + count_x + count_z + planes0 + count_g + late_packs + planes1:
        m.wait_send()
    for part in PARTS:
        for m in moves[part]:
            m.wait_send()


N_MESSAGES = (NX - 1) + (NZ - 1) + 2 + 2 + 2 + 6 + 6 + 2 * len(PARTS)


def local(state, coef, counts):
    f32, i32 = jnp.float32, jnp.int32
    vmem = pltpu.VMEM
    result = pl.pallas_call(
        kernel,
        out_shape=vmem((8, 8, 64, 128), f32),
        in_specs=[
            pl.BlockSpec(memory_space=pltpu.SMEM),
            pl.BlockSpec(memory_space=pl.ANY),
            pl.BlockSpec(memory_space=pl.ANY),
        ],
        out_specs=pl.BlockSpec(memory_space=vmem),
        scratch_shapes=[
            vmem((8, 8, 96, 128), f32), vmem((8, 8, 96, 128), f32), vmem((8, 8, 96, 128), f32),
            vmem((10, 8, CH, 8, 128), f32), vmem((10, 8, CH, 8, 128), f32), vmem((8, 8, CH, 8, 128), f32),
            vmem((2, 8, CH, 8, 128), f32),
            vmem((2, 8, 25, 8, 128), f32), vmem((2, 8, 25, 8, 128), f32),
            vmem((2, 8, 4, 8, 128), f32), vmem((2, 8, 4, 8, 128), f32),
            vmem((2, 4, 8, 128), f32), vmem((2, 4, 8, 128), f32),
            vmem((2, 8, 128), f32), vmem((2, 8, 128), f32),
            vmem((8, 8, 2, 8, 128), f32), vmem((8, 8, 2, 8, 128), f32),
            vmem((8, 8, 2, 8, 128), f32), vmem((8, 8, 2, 8, 128), f32),
            vmem((8, 8, 17, 8, 128), f32),
            vmem((NX, 1, 128), i32), vmem((NZ, NX, 1, 128), i32), vmem((2, 8, 128), i32), vmem((1, 128), i32), vmem((8, 128), i32),
            pltpu.SemaphoreType.DMA((3, 8)),
            pltpu.SemaphoreType.DMA((N_MESSAGES,)), pltpu.SemaphoreType.DMA((N_MESSAGES,)),
        ],
        compiler_params=pltpu.CompilerParams(
            collective_id=0, has_side_effects=True, vmem_limit_bytes=60 * 1024 * 1024),
    )(counts, state.reshape(2, 8, 8, 96, 128), coef.reshape(8, 8, 96, 128))
    return result.reshape(512, 1, AVG)


def solution(mesh):
    placed = (P(None, None, "grp", "curve"), P(None, "grp", "curve"), P("grp", "curve"))
    return jax.shard_map(
        local, mesh=mesh, in_specs=placed, out_specs=P(None, "grp", "curve"), check_vma=False
    )
```

```python
import jax
import jax.numpy as jnp
from jax import lax
from jax.experimental import pallas as pl
from jax.experimental.pallas import tpu as pltpu
from jax.sharding import PartitionSpec as P

AVG = 1024
HALF = 256
CAP = 1536
NX, NZ = 4, 8
N_CURVE = NX * NZ
N_GRP = 8
CH = CAP // 128
MESH = pl.DeviceIdType.MESH
ORDER = (2, 3, 4, 5, 1, 6, 0, 7)
INNER, MIDDLE, EDGE_LOW, EDGE_HIGH, NEXT, LAST_LOW, LAST_HIGH = PARTS = (
    (0, 4, 2, 2), (0, 4, 4, 2), (0, 4, 0, 2), (0, 4, 6, 2), (4, 2, 0, 8), (6, 1, 0, 8), (7, 1, 0, 8),
)


class Message:
    def __init__(self, make, sends, receives):
        self.make, self.sends, self.receives = make, sends, receives

    def start(self):
        pl.when(self.sends)(lambda: self.make().start())

    def wait_recv(self):
        pl.when(self.receives)(lambda: self.make().wait_recv())

    def wait_send(self):
        pl.when(self.sends)(lambda: self.make().wait_send())


def kernel(
    counts, state, coef, out,
    raw_u, raw_s, raw_c, u0, u1, inv, yh, rx0_low, rx0_high, rx1_low, rx1_high, ts0, ts1, ps, pr, ls, lr,
    t2s, t2r, h2s, h2r, wide, cbx, cbz, cb3, cs, cs3,

    in_sem, send_sem, recv_sem,
):
    rank, grp = lax.axis_index("curve"), lax.axis_index("grp")
    xc, zc = rank // NZ, rank % NZ
    has_left, has_right = rank > 0, rank < N_CURVE - 1
    has_low, has_high = grp > 0, grp < N_GRP - 1
    left, right = (rank + N_CURVE - 1) % N_CURVE, (rank + 1) % N_CURVE
    low, high = (grp + N_GRP - 1) % N_GRP, (grp + 1) % N_GRP

    barrier = pltpu.get_barrier_semaphore()
    peers = [(r, g) for g in (low, high) for r in (left, rank, right)]
    peers += [(left, grp), (right, grp)]
    peers += [(((xc + k) % NX) * NZ + zc, grp) for k in range(1, NX)]
    peers += [(xc * NZ + (zc + k) % NZ, grp) for k in range(1, NZ)]
    loads = {}
    for kind, src, dst in ((0, state.at[0], raw_u), (1, state.at[1], raw_s), (2, coef, raw_c)):
        for x in range(8):
            loads[kind, x] = pltpu.make_async_copy(src.at[x], dst.at[x], in_sem.at[kind, x])
    first_loads = [(0, x) for x in range(8)] + [(1, 0), (1, 7), (2, 0), (2, 7)]
    other_loads = [(kind, x) for x in range(1, 7) for kind in (1, 2)]
    for key in first_loads:
        loads[key].start()
    for peer in peers:
        pl.semaphore_signal(barrier, inc=1, device_id=peer, device_id_type=MESH)

    lane = lax.broadcasted_iota(jnp.int32, (8, 128), 1)
    sub = lax.broadcasted_iota(jnp.int32, (8, 128), 0)
    zero = jnp.zeros((8, 128), jnp.float32)
    held = counts[0, 0]

    rx0, rx1 = (rx0_low, rx0_high), (rx1_low, rx1_high)
    index = [0]

    def message(src, dst, device, sends, receives):
        at = index[0]
        index[0] += 1

        def make():
            return pltpu.make_async_remote_copy(
                src_ref=src(), dst_ref=dst(), send_sem=send_sem.at[at], recv_sem=recv_sem.at[at],
                device_id=device, device_id_type=MESH,
            )

        return Message(make, sends, receives)

    yes = rank >= 0
    count_x = [
        message(lambda: cs, lambda: cbx.at[xc], (((xc + k) % NX) * NZ + zc, grp), yes, yes)
        for k in range(1, NX)
    ]
    count_z = [
        message(lambda: cbx, lambda: cbz.at[zc], (xc * NZ + (zc + k) % NZ, grp), yes, yes)
        for k in range(1, NZ)
    ]
    count_g = [
        message(lambda: cs3, lambda: cb3.at[1], (rank, low), has_low, has_high),
        message(lambda: cs3, lambda: cb3.at[0], (rank, high), has_high, has_low),
    ]
    packs = [
        message(lambda: ps.at[0], lambda: pr.at[1], (left, grp), has_left, has_right),
        message(lambda: ps.at[1], lambda: pr.at[0], (right, grp), has_right, has_left),
    ]
    late_packs = [
        message(lambda: ls.at[0], lambda: lr.at[1], (left, grp), has_left, has_right),
        message(lambda: ls.at[1], lambda: lr.at[0], (right, grp), has_right, has_left),
    ]

    def planes_out(u, ts, rx):
        tails, heads, mids = [], [], []
        for d, y, other, sends, receives in (
            (0, 0, low, has_low, has_high), (1, 7, high, has_high, has_low),
        ):
            tails.append(message(
                lambda d=d: ts.at[d], lambda d=d: rx[1 - d].at[:, pl.ds(0, 4)], (right, other),
                jnp.logical_and(sends, has_right), jnp.logical_and(receives, has_left)))
            heads.append(message(
                lambda y=y: u.at[pl.ds(1, 8), y, pl.ds(0, 4)],
                lambda d=d: rx[1 - d].at[:, pl.ds(16, 4)], (left, other),
                jnp.logical_and(sends, has_left), jnp.logical_and(receives, has_right)))
            mids.append(message(
                lambda y=y: u.at[pl.ds(1, 8), y], lambda d=d: rx[1 - d].at[:, pl.ds(4, 12)],
                (rank, other), sends, receives))
        return [tails[0], heads[0]], mids, [tails[1], heads[1]]

    planes0_low, planes0_mid, planes0_high = planes_out(u0, ts0, rx0)
    planes0 = planes0_low + planes0_mid + planes0_high
    planes1_low, planes1_mid, planes1_high = planes_out(u1, ts1, rx1)
    planes1 = planes1_low + planes1_mid[:1] + planes1_high + planes1_mid[1:]
    moves = {}
    for part in PARTS:
        at = (pl.ds(part[0], part[1]), pl.ds(part[2], part[3]))
        moves[part] = [
            message(lambda at=at: t2s.at[at], lambda at=at: t2r.at[at], (right, grp), has_right, has_left),
            message(lambda at=at: h2s.at[at], lambda at=at: h2r.at[at], (left, grp), has_left, has_right),
        ]

    def loop(start, stop, body, unroll=1):
        if unroll == stop - start:
            for x in range(start, stop):
                body(x)
            return

        def step(i, carry):
            for k in range(unroll):
                body(start + i * unroll + k)
            return carry

        lax.fori_loop(0, (stop - start) // unroll, step, 0)

    def rolled(value, turn):
        return pltpu.roll(value, turn, 1)

    def shifted(load, start, chunks, lowest, highest):
        first, offset = jnp.clip(start >> 7, lowest, highest), start & 127
        turn = (128 - offset) & 127
        turned = {}
        for k in sorted(set(chunks) | {k + 1 for k in chunks}):
            turned[k] = rolled(load(first + k), turn)
        keep = lane < 128 - offset
        return {k: jnp.where(keep, turned[k], turned[k + 1]) for k in chunks}

    def convert(x):
        for y in range(8):
            for c in range(CH):
                u0[x + 1, y, c] = raw_u[x, y, pl.ds(c, 8, stride=CH), :]

    def plane_tails(u, ts):
        def body(x):
            for d, y in ((0, 0), (1, 7)):
                got = shifted(
                    lambda k: u[x + 1, y, jnp.minimum(k, CH - 1)], held - 512, range(4), 0, 8)
                for k in range(4):
                    ts[d, x, k] = got[k]

        loop(0, 8, body, 8)

    last_chunk, last_lane = jnp.clip((held - 1) >> 7, 0, CH - 1), (held - 1) & 127

    def lanes_packed(load, at, ys):
        acc = zero
        for y in ys:
            acc = jnp.where(lane == y, rolled(load(y), (y - at) & 127) if not isinstance(at, int) else pltpu.roll(load(y), (y - at) & 127, 1), acc)
        return acc

    def first_of(u, x, ys):
        return lanes_packed(lambda y: u[x + 1, y, 0], 0, ys)

    def last_of(u, x, ys):
        return lanes_packed(lambda y: u[x + 1, y, last_chunk], last_lane, ys)

    def fill_x(u, left_tile, right_tile, ys):
        for y in ys:
            from_left = jnp.broadcast_to(left_tile[:, y : y + 1], (8, 128))
            from_right = jnp.broadcast_to(right_tile[:, y : y + 1], (8, 128))
            turned = [pltpu.roll(u[1, y, c], 127, 1) for c in range(CH)]
            for c in range(CH):
                value = jnp.where(lane < 127, turned[c], turned[min(c + 1, CH - 1)])
                u[9, y, c] = jnp.where(lane + 128 * c == held - 1, from_right, value)
            turned = [pltpu.roll(u[8, y, c], 1, 1) for c in range(CH)]
            for c in range(CH):
                u[0, y, c] = jnp.where(lane > 0, turned[c], turned[c - 1] if c else from_left)

    def along_z(value):
        up = jnp.where(sub < 7, pltpu.roll(value, 7, 0), 0.0)
        down = jnp.where(sub > 0, pltpu.roll(value, 1, 0), 0.0)
        return up + down

    def sweep(u, first, ys, store, xs=(0, 8, 1)):
        need = sorted({y + d for y in ys for d in (-1, 0, 1)} & set(range(8)))

        def body(x):
            for c in range(CH):
                here = {y: u[x + 1, y, c] for y in need}
                here[-1] = yh[0, x, c] if 0 in ys else None
                here[8] = yh[1, x, c] if 7 in ys else None
                for y in ys:
                    total = u[x, y, c] + u[x + 2, y, c]
                    total = total + (here[y - 1] + here[y + 1]) + along_z(here[y])
                    if first:
                        scale = 1.0 / (6.0 + raw_c[x, y, pl.ds(c, 8, stride=CH), :])
                        inv[x, y, c] = scale
                    else:
                        scale = inv[x, y, c]
                    store(x, y, c, (raw_s[x, y, pl.ds(c, 8, stride=CH), :] + total) * scale)

        loop(xs[0], xs[1], body, xs[2])

    def store_u1(x, y, c, value):
        u1[x + 1, y, c] = value

    def store_wide(x, y, c, value):
        wide[x, y, c + 2] = value

    def move(part):
        start, size, x_start, x_size = part

        def body(x):
            for p in range(start, start + size):
                y = ORDER[p]
                got = shifted(lambda k: wide[x, y, k + 2], held - HALF, range(2), 2, 10)
                for k in range(2):
                    t2s[p, x, k] = got[k]
                    h2s[p, x, k] = wide[x, y, k + 2]

        loop(x_start, x_start + x_size, body, x_size)

    def halos(rx, drift_prev, sides=(0, 1)):
        starts = {}
        for side in sides:
            tile = cb3[side]
            other_prev = tile[0, 0] - rank * AVG
            other_next = tile[1, 0] - (rank + 1) * AVG
            starts[side] = (AVG // 2 + drift_prev - other_prev, AVG + drift_prev - other_next)

        def body(x):
            for side in sides:
                exists = (has_low, has_high)[side]
                load = lambda k: rx[side][x, k]
                begin, begin_next = starts[side]
                own = shifted(load, begin, range(CH), 0, 8)
                later = shifted(load, begin_next, range(4, CH), 4, 12)
                for c in range(CH):
                    value = own[c]
                    if c >= 4:
                        value = jnp.where(lane + 128 * c >= 2 * AVG - begin_next, later[c], value)
                    yh[side, x, c] = jnp.where(exists, value, zero)

        loop(0, 8, body, 8 // len(sides))

    def finish(part, drift_prev, drift_next):
        for m in moves[part]:
            m.wait_recv()
        start, size, x_start, x_size = part

        def body(x):
            for p in range(start, start + size):
                y = ORDER[p]
                for k in range(2):
                    wide[x, y, k] = t2r[p, x, k]
                    wide[x, y, 14 + k] = h2r[p, x, k]
                load = lambda k: wide[x, y, k]
                own = shifted(load, HALF - drift_prev, range(8), 0, 4)
                later = shifted(load, 768 - drift_next, range(6, 8), 4, 8)
                for k in range(8):
                    value = own[k]
                    if k >= 6:
                        value = jnp.where(lane + 128 * k >= AVG + drift_next, later[k], value)
                    out[x, y, pl.ds(k, 8, stride=8), :] = value

        loop(x_start, x_start + x_size, body, min(x_size, 8 // size))

    for key in first_loads[:4]:
        loads[key].wait()
    for key in other_loads:
        loads[key].start()
    for key in first_loads[4:8]:
        loads[key].wait()
    loop(0, 8, convert)
    cs[...] = jnp.full((1, 128), held, jnp.int32)
    cbx[xc] = jnp.full((1, 128), held, jnp.int32)
    plane_tails(u0, ts0)
    for key in first_loads[8:]:
        loads[key].wait()
    every = range(8)
    ps[0, 0] = first_of(u0, 0, every)
    ps[0, 1] = first_of(u0, 1, every)
    ps[1, 0] = last_of(u0, 7, every)
    ps[1, 1] = last_of(u0, 6, every)
    for k, raw in ((2, raw_s), (3, raw_c)):
        ps[0, k] = lanes_packed(lambda y: raw[0, y, pl.ds(0, 8, stride=CH), :], 0, every)

        def last_tile(y):
            tile = raw[7, y, pl.ds(0, 8, stride=CH), :]
            for c in range(1, CH):
                tile = jnp.where(last_chunk == c, raw[7, y, pl.ds(c, 8, stride=CH), :], tile)
            return tile

        ps[1, k] = lanes_packed(last_tile, last_lane, every)

    pl.semaphore_wait(barrier, len(peers))
    for m in count_x + packs + planes0_low + planes0_mid:
        m.start()

    for key in other_loads:
        loads[key].wait()
    sweep(u0, True, range(1, 7), store_u1, (1, 7, 1))
    sweep(u1, False, range(2, 6), store_wide, (2, 6, 1))
    move(INNER)
    for m in moves[INNER]:
        m.start()
    move(MIDDLE)
    for m in count_x:
        m.wait_recv()
    for m in count_z + planes0_high + moves[MIDDLE]:
        m.start()
    for m in packs:
        m.wait_recv()
    left0 = jnp.where(has_left, pr[0, 0], zero)
    right0 = jnp.where(has_right, pr[1, 0], zero)
    fill_x(u0, left0, right0, every)
    sweep(u0, True, range(1, 7), store_u1, (0, 1, 1))
    sweep(u0, True, range(1, 7), store_u1, (7, 8, 1))

    def edge_u1(side, own, exists):
        u = pr[side, 0]
        along_y = jnp.where(lane < 7, pltpu.roll(u, 127, 1), 0.0) + jnp.where(lane > 0, pltpu.roll(u, 1, 1), 0.0)
        total = pr[side, 1] + own + along_y + along_z(u)
        return jnp.where(exists, (pr[side, 2] + total) / (6.0 + pr[side, 3]), zero)

    left1 = edge_u1(0, ps[0, 0], has_left)
    right1 = edge_u1(1, ps[1, 0], has_right)
    fill_x(u1, left1, right1, range(1, 7))
    sweep(u1, False, range(2, 6), store_wide, (0, 2, 1))
    move(EDGE_LOW)
    for m in moves[EDGE_LOW]:
        m.start()
    sweep(u1, False, range(2, 6), store_wide, (6, 8, 1))
    move(EDGE_HIGH)
    for m in moves[EDGE_HIGH]:
        m.start()

    for m in count_z:
        m.wait_recv()
    before = jnp.zeros((1, 128), jnp.int32)
    for x in range(NX):
        for z in range(NZ):
            row = jnp.where(z == zc, cbx[x], cbz[z, x])
            before = before + jnp.where(x * NZ + z < rank, row, 0)
    drift_prev = before[0, 0] - rank * AVG
    drift_next = drift_prev + held - AVG
    cs3[...] = jnp.where(sub == 0, before, before + held)
    for m in count_g:
        m.start()

    for m in planes0 + count_g:
        m.wait_recv()
    halos(rx0, drift_prev)
    sweep(u0, True, (0, 7), store_u1)
    plane_tails(u1, ts1)
    ls[0] = first_of(u1, 0, (0, 7))
    ls[1] = last_of(u1, 7, (0, 7))
    for m in late_packs + planes1:
        m.start()

    sweep(u1, False, (1, 6), store_wide)
    move(NEXT)
    for m in moves[NEXT]:
        m.start()
    for part in (INNER, MIDDLE, EDGE_LOW, EDGE_HIGH):
        finish(part, drift_prev, drift_next)

    for m in late_packs:
        m.wait_recv()
    fill_x(u1, jnp.where(has_left, lr[0], zero), jnp.where(has_right, lr[1], zero), (0, 7))
    for m in planes1[:3]:
        m.wait_recv()
    halos(rx1, drift_prev, (1,))
    sweep(u1, False, (7,), store_wide, (0, 8, 2))
    move(LAST_HIGH)
    for m in moves[LAST_HIGH]:
        m.start()
    for m in planes1[3:]:
        m.wait_recv()
    halos(rx1, drift_prev, (0,))
    sweep(u1, False, (0,), store_wide, (0, 8, 2))
    move(LAST_LOW)
    for m in moves[LAST_LOW]:
        m.start()
    for part in (NEXT, LAST_HIGH, LAST_LOW):
        finish(part, drift_prev, drift_next)

    for m in packs + count_x + count_z + planes0 + count_g + late_packs + planes1:
        m.wait_send()
    for part in PARTS:
        for m in moves[part]:
            m.wait_send()


N_MESSAGES = (NX - 1) + (NZ - 1) + 2 + 2 + 2 + 6 + 6 + 2 * len(PARTS)


def local(state, coef, counts):
    f32, i32 = jnp.float32, jnp.int32
    vmem = pltpu.VMEM
    result = pl.pallas_call(
        kernel,
        out_shape=vmem((8, 8, 64, 128), f32),
        in_specs=[
            pl.BlockSpec(memory_space=pltpu.SMEM),
            pl.BlockSpec(memory_space=pl.ANY),
            pl.BlockSpec(memory_space=pl.ANY),
        ],
        out_specs=pl.BlockSpec(memory_space=vmem),
        scratch_shapes=[
            vmem((8, 8, 96, 128), f32), vmem((8, 8, 96, 128), f32), vmem((8, 8, 96, 128), f32),
            vmem((10, 8, CH, 8, 128), f32), vmem((10, 8, CH, 8, 128), f32), vmem((8, 8, CH, 8, 128), f32),
            vmem((2, 8, CH, 8, 128), f32),
            vmem((8, 25, 8, 128), f32), vmem((8, 25, 8, 128), f32), vmem((8, 25, 8, 128), f32), vmem((8, 25, 8, 128), f32),
            vmem((2, 8, 4, 8, 128), f32), vmem((2, 8, 4, 8, 128), f32),
            vmem((2, 4, 8, 128), f32), vmem((2, 4, 8, 128), f32),
            vmem((2, 8, 128), f32), vmem((2, 8, 128), f32),
            vmem((8, 8, 2, 8, 128), f32), vmem((8, 8, 2, 8, 128), f32),
            vmem((8, 8, 2, 8, 128), f32), vmem((8, 8, 2, 8, 128), f32),
            vmem((8, 8, 17, 8, 128), f32),
            vmem((NX, 1, 128), i32), vmem((NZ, NX, 1, 128), i32), vmem((2, 8, 128), i32), vmem((1, 128), i32), vmem((8, 128), i32),
            pltpu.SemaphoreType.DMA((3, 8)),
            pltpu.SemaphoreType.DMA((N_MESSAGES,)), pltpu.SemaphoreType.DMA((N_MESSAGES,)),
        ],
        compiler_params=pltpu.CompilerParams(
            collective_id=0, has_side_effects=True, vmem_limit_bytes=60 * 1024 * 1024),
    )(counts, state.reshape(2, 8, 8, 96, 128), coef.reshape(8, 8, 96, 128))
    return result.reshape(512, 1, AVG)


def solution(mesh):
    placed = (P(None, None, "grp", "curve"), P(None, "grp", "curve"), P("grp", "curve"))
    return jax.shard_map(
        local, mesh=mesh, in_specs=placed, out_specs=P(None, "grp", "curve"), check_vma=False
    )
```

```python
import jax
import jax.numpy as jnp
from jax import lax
from jax.experimental import pallas as pl
from jax.experimental.pallas import tpu as pltpu
from jax.sharding import PartitionSpec as P

AVG = 1024
HALF = 256
CAP = 1536
NX, NZ = 4, 8
N_CURVE = NX * NZ
N_GRP = 8
CH = CAP // 128
MESH = pl.DeviceIdType.MESH
ORDER = (2, 3, 4, 5, 1, 6, 0, 7)
INNER, MIDDLE, EDGE_LOW, EDGE_HIGH, NEXT, LOW_A, LOW_B, HIGH_A, HIGH_B = PARTS = (
    (0, 4, 2, 2), (0, 4, 4, 2), (0, 4, 0, 2), (0, 4, 6, 2), (4, 2, 0, 8),
    (6, 1, 0, 4), (6, 1, 4, 4), (7, 1, 0, 4), (7, 1, 4, 4),
)


class Message:
    def __init__(self, make, sends, receives):
        self.make, self.sends, self.receives = make, sends, receives

    def start(self):
        pl.when(self.sends)(lambda: self.make().start())

    def wait_recv(self):
        pl.when(self.receives)(lambda: self.make().wait_recv())

    def wait_send(self):
        pl.when(self.sends)(lambda: self.make().wait_send())


def kernel(
    counts, state, coef, out,
    raw_u, raw_s, raw_c, u0, u1, inv, yh, rx0_low, rx0_high, rx1_low, rx1_high, ts0, ts1, ps, pr, ls, lr,
    t2s, t2r, h2s, h2r, wide, cbx, cbz, cb3, cs, cs3,

    in_sem, send_sem, recv_sem,
):
    rank, grp = lax.axis_index("curve"), lax.axis_index("grp")
    xc, zc = rank // NZ, rank % NZ
    has_left, has_right = rank > 0, rank < N_CURVE - 1
    has_low, has_high = grp > 0, grp < N_GRP - 1
    left, right = (rank + N_CURVE - 1) % N_CURVE, (rank + 1) % N_CURVE
    low, high = (grp + N_GRP - 1) % N_GRP, (grp + 1) % N_GRP

    barrier = pltpu.get_barrier_semaphore()
    peers = [(r, g) for g in (low, high) for r in (left, rank, right)]
    peers += [(left, grp), (right, grp)]
    peers += [(((xc + k) % NX) * NZ + zc, grp) for k in range(1, NX)]
    peers += [(xc * NZ + (zc + k) % NZ, grp) for k in range(1, NZ)]
    loads = {}
    for kind, src, dst in ((0, state.at[0], raw_u), (1, state.at[1], raw_s), (2, coef, raw_c)):
        for x in range(8):
            loads[kind, x] = pltpu.make_async_copy(src.at[x], dst.at[x], in_sem.at[kind, x])
    first_loads = [(0, x) for x in range(8)] + [(1, 0), (1, 7), (2, 0), (2, 7)]
    other_loads = [(kind, x) for x in range(1, 7) for kind in (1, 2)]
    for key in first_loads:
        loads[key].start()
    for peer in peers:
        pl.semaphore_signal(barrier, inc=1, device_id=peer, device_id_type=MESH)

    lane = lax.broadcasted_iota(jnp.int32, (8, 128), 1)
    sub = lax.broadcasted_iota(jnp.int32, (8, 128), 0)
    zero = jnp.zeros((8, 128), jnp.float32)
    held = counts[0, 0]

    rx0, rx1 = (rx0_low, rx0_high), (rx1_low, rx1_high)
    index = [0]

    def message(src, dst, device, sends, receives):
        at = index[0]
        index[0] += 1

        def make():
            return pltpu.make_async_remote_copy(
                src_ref=src(), dst_ref=dst(), send_sem=send_sem.at[at], recv_sem=recv_sem.at[at],
                device_id=device, device_id_type=MESH,
            )

        return Message(make, sends, receives)

    yes = rank >= 0
    count_x = [
        message(lambda: cs, lambda: cbx.at[xc], (((xc + k) % NX) * NZ + zc, grp), yes, yes)
        for k in range(1, NX)
    ]
    count_z = [
        message(lambda: cbx, lambda: cbz.at[zc], (xc * NZ + (zc + k) % NZ, grp), yes, yes)
        for k in range(1, NZ)
    ]
    count_g = [
        message(lambda: cs3, lambda: cb3.at[1], (rank, low), has_low, has_high),
        message(lambda: cs3, lambda: cb3.at[0], (rank, high), has_high, has_low),
    ]
    packs = [
        message(lambda: ps.at[0], lambda: pr.at[1], (left, grp), has_left, has_right),
        message(lambda: ps.at[1], lambda: pr.at[0], (right, grp), has_right, has_left),
    ]
    late_packs = [
        message(lambda: ls.at[0], lambda: lr.at[1], (left, grp), has_left, has_right),
        message(lambda: ls.at[1], lambda: lr.at[0], (right, grp), has_right, has_left),
    ]

    def planes_out(u, ts, rx):
        tails, heads, mids = [], [], []
        for d, y, other, sends, receives in (
            (0, 0, low, has_low, has_high), (1, 7, high, has_high, has_low),
        ):
            tails.append(message(
                lambda d=d: ts.at[d], lambda d=d: rx[1 - d].at[:, pl.ds(0, 4)], (right, other),
                jnp.logical_and(sends, has_right), jnp.logical_and(receives, has_left)))
            heads.append(message(
                lambda y=y: u.at[pl.ds(1, 8), y, pl.ds(0, 4)],
                lambda d=d: rx[1 - d].at[:, pl.ds(16, 4)], (left, other),
                jnp.logical_and(sends, has_left), jnp.logical_and(receives, has_right)))
            mids.append(message(
                lambda y=y: u.at[pl.ds(1, 8), y], lambda d=d: rx[1 - d].at[:, pl.ds(4, 12)],
                (rank, other), sends, receives))
        return [tails[0], heads[0]], mids, [tails[1], heads[1]]

    planes0_low, planes0_mid, planes0_high = planes_out(u0, ts0, rx0)
    planes0 = planes0_low + planes0_mid + planes0_high
    planes1_low, planes1_mid, planes1_high = planes_out(u1, ts1, rx1)
    planes1 = planes1_low + planes1_mid[:1] + planes1_high + planes1_mid[1:]
    moves = {}
    for part in PARTS:
        at = (pl.ds(part[0], part[1]), pl.ds(part[2], part[3]))
        moves[part] = [
            message(lambda at=at: t2s.at[at], lambda at=at: t2r.at[at], (right, grp), has_right, has_left),
            message(lambda at=at: h2s.at[at], lambda at=at: h2r.at[at], (left, grp), has_left, has_right),
        ]

    def loop(start, stop, body, unroll=1):
        if unroll == stop - start:
            for x in range(start, stop):
                body(x)
            return

        def step(i, carry):
            for k in range(unroll):
                body(start + i * unroll + k)
            return carry

        lax.fori_loop(0, (stop - start) // unroll, step, 0)

    def rolled(value, turn):
        return pltpu.roll(value, turn, 1)

    def shifted(load, start, chunks, lowest, highest):
        first, offset = jnp.clip(start >> 7, lowest, highest), start & 127
        turn = (128 - offset) & 127
        turned = {}
        for k in sorted(set(chunks) | {k + 1 for k in chunks}):
            turned[k] = rolled(load(first + k), turn)
        keep = lane < 128 - offset
        return {k: jnp.where(keep, turned[k], turned[k + 1]) for k in chunks}

    def convert(x):
        for y in range(8):
            for c in range(CH):
                u0[x + 1, y, c] = raw_u[x, y, pl.ds(c, 8, stride=CH), :]

    def plane_tails(u, ts):
        def body(x):
            for d, y in ((0, 0), (1, 7)):
                got = shifted(
                    lambda k: u[x + 1, y, jnp.minimum(k, CH - 1)], held - 512, range(4), 0, 8)
                for k in range(4):
                    ts[d, x, k] = got[k]

        loop(0, 8, body, 8)

    last_chunk, last_lane = jnp.clip((held - 1) >> 7, 0, CH - 1), (held - 1) & 127

    def lanes_packed(load, at, ys):
        acc = zero
        for y in ys:
            acc = jnp.where(lane == y, rolled(load(y), (y - at) & 127) if not isinstance(at, int) else pltpu.roll(load(y), (y - at) & 127, 1), acc)
        return acc

    def first_of(u, x, ys):
        return lanes_packed(lambda y: u[x + 1, y, 0], 0, ys)

    def last_of(u, x, ys):
        return lanes_packed(lambda y: u[x + 1, y, last_chunk], last_lane, ys)

    def fill_x(u, left_tile, right_tile, ys):
        for y in ys:
            from_left = jnp.broadcast_to(left_tile[:, y : y + 1], (8, 128))
            from_right = jnp.broadcast_to(right_tile[:, y : y + 1], (8, 128))
            turned = [pltpu.roll(u[1, y, c], 127, 1) for c in range(CH)]
            for c in range(CH):
                value = jnp.where(lane < 127, turned[c], turned[min(c + 1, CH - 1)])
                u[9, y, c] = jnp.where(lane + 128 * c == held - 1, from_right, value)
            turned = [pltpu.roll(u[8, y, c], 1, 1) for c in range(CH)]
            for c in range(CH):
                u[0, y, c] = jnp.where(lane > 0, turned[c], turned[c - 1] if c else from_left)

    def along_z(value):
        up = jnp.where(sub < 7, pltpu.roll(value, 7, 0), 0.0)
        down = jnp.where(sub > 0, pltpu.roll(value, 1, 0), 0.0)
        return up + down

    def sweep(u, first, ys, store, xs=(0, 8, 1)):
        need = sorted({y + d for y in ys for d in (-1, 0, 1)} & set(range(8)))

        def body(x):
            for c in range(CH):
                here = {y: u[x + 1, y, c] for y in need}
                here[-1] = yh[0, x, c] if 0 in ys else None
                here[8] = yh[1, x, c] if 7 in ys else None
                for y in ys:
                    total = u[x, y, c] + u[x + 2, y, c]
                    total = total + (here[y - 1] + here[y + 1]) + along_z(here[y])
                    if first:
                        scale = 1.0 / (6.0 + raw_c[x, y, pl.ds(c, 8, stride=CH), :])
                        inv[x, y, c] = scale
                    else:
                        scale = inv[x, y, c]
                    store(x, y, c, (raw_s[x, y, pl.ds(c, 8, stride=CH), :] + total) * scale)

        loop(xs[0], xs[1], body, xs[2])

    def store_u1(x, y, c, value):
        u1[x + 1, y, c] = value

    def store_wide(x, y, c, value):
        wide[x, y, c + 2] = value

    def move(part):
        start, size, x_start, x_size = part

        def body(x):
            for p in range(start, start + size):
                y = ORDER[p]
                got = shifted(lambda k: wide[x, y, k + 2], held - HALF, range(2), 2, 10)
                for k in range(2):
                    t2s[p, x, k] = got[k]
                    h2s[p, x, k] = wide[x, y, k + 2]

        loop(x_start, x_start + x_size, body, x_size)

    def halos(rx, drift_prev, sides=(0, 1)):
        starts = {}
        for side in sides:
            tile = cb3[side]
            other_prev = tile[0, 0] - rank * AVG
            other_next = tile[1, 0] - (rank + 1) * AVG
            starts[side] = (AVG // 2 + drift_prev - other_prev, AVG + drift_prev - other_next)

        def body(x):
            for side in sides:
                exists = (has_low, has_high)[side]
                load = lambda k: rx[side][x, k]
                begin, begin_next = starts[side]
                own = shifted(load, begin, range(CH), 0, 8)
                later = shifted(load, begin_next, range(4, CH), 4, 12)
                for c in range(CH):
                    value = own[c]
                    if c >= 4:
                        value = jnp.where(lane + 128 * c >= 2 * AVG - begin_next, later[c], value)
                    yh[side, x, c] = jnp.where(exists, value, zero)

        loop(0, 8, body, 8 // len(sides))

    def finish(part, drift_prev, drift_next):
        for m in moves[part]:
            m.wait_recv()
        start, size, x_start, x_size = part

        def body(x):
            for p in range(start, start + size):
                y = ORDER[p]
                for k in range(2):
                    wide[x, y, k] = t2r[p, x, k]
                    wide[x, y, 14 + k] = h2r[p, x, k]
                load = lambda k: wide[x, y, k]
                own = shifted(load, HALF - drift_prev, range(8), 0, 4)
                later = shifted(load, 768 - drift_next, range(6, 8), 4, 8)
                for k in range(8):
                    value = own[k]
                    if k >= 6:
                        value = jnp.where(lane + 128 * k >= AVG + drift_next, later[k], value)
                    out[x, y, pl.ds(k, 8, stride=8), :] = value

        loop(x_start, x_start + x_size, body, min(x_size, 8 // size))

    for key in first_loads[:4]:
        loads[key].wait()
    for key in other_loads:
        loads[key].start()
    for key in first_loads[4:8]:
        loads[key].wait()
    loop(0, 8, convert)
    cs[...] = jnp.full((1, 128), held, jnp.int32)
    cbx[xc] = jnp.full((1, 128), held, jnp.int32)
    plane_tails(u0, ts0)
    for key in first_loads[8:]:
        loads[key].wait()
    every = range(8)
    ps[0, 0] = first_of(u0, 0, every)
    ps[0, 1] = first_of(u0, 1, every)
    ps[1, 0] = last_of(u0, 7, every)
    ps[1, 1] = last_of(u0, 6, every)
    for k, raw in ((2, raw_s), (3, raw_c)):
        ps[0, k] = lanes_packed(lambda y: raw[0, y, pl.ds(0, 8, stride=CH), :], 0, every)

        def last_tile(y):
            tile = raw[7, y, pl.ds(0, 8, stride=CH), :]
            for c in range(1, CH):
                tile = jnp.where(last_chunk == c, raw[7, y, pl.ds(c, 8, stride=CH), :], tile)
            return tile

        ps[1, k] = lanes_packed(last_tile, last_lane, every)

    pl.semaphore_wait(barrier, len(peers))
    for m in count_x + packs + planes0_low + planes0_mid:
        m.start()
    for key in other_loads:
        loads[key].wait()
    sweep(u0, True, range(1, 7), store_u1, (1, 7, 1))
    sweep(u1, False, range(2, 6), store_wide, (2, 6, 1))
    move(INNER)
    for m in moves[INNER]:
        m.start()
    move(MIDDLE)
    for m in count_x:
        m.wait_recv()
    for m in count_z + planes0_high + moves[MIDDLE]:
        m.start()
    for m in packs:
        m.wait_recv()
    left0 = jnp.where(has_left, pr[0, 0], zero)
    right0 = jnp.where(has_right, pr[1, 0], zero)
    fill_x(u0, left0, right0, every)
    sweep(u0, True, range(1, 7), store_u1, (0, 1, 1))
    sweep(u0, True, range(1, 7), store_u1, (7, 8, 1))

    def edge_u1(side, own, exists):
        u = pr[side, 0]
        along_y = jnp.where(lane < 7, pltpu.roll(u, 127, 1), 0.0) + jnp.where(lane > 0, pltpu.roll(u, 1, 1), 0.0)
        total = pr[side, 1] + own + along_y + along_z(u)
        return jnp.where(exists, (pr[side, 2] + total) / (6.0 + pr[side, 3]), zero)

    left1 = edge_u1(0, ps[0, 0], has_left)
    right1 = edge_u1(1, ps[1, 0], has_right)
    fill_x(u1, left1, right1, range(1, 7))
    sweep(u1, False, range(2, 6), store_wide, (0, 2, 1))
    move(EDGE_LOW)
    for m in moves[EDGE_LOW]:
        m.start()
    sweep(u1, False, range(2, 6), store_wide, (6, 8, 1))
    move(EDGE_HIGH)
    for m in moves[EDGE_HIGH]:
        m.start()

    for m in count_z:
        m.wait_recv()
    before = jnp.zeros((1, 128), jnp.int32)
    for x in range(NX):
        for z in range(NZ):
            row = jnp.where(z == zc, cbx[x], cbz[z, x])
            before = before + jnp.where(x * NZ + z < rank, row, 0)
    drift_prev = before[0, 0] - rank * AVG
    drift_next = drift_prev + held - AVG
    cs3[...] = jnp.where(sub == 0, before, before + held)
    for m in count_g:
        m.start()

    for m in planes0 + count_g:
        m.wait_recv()
    halos(rx0, drift_prev)
    sweep(u0, True, (0, 7), store_u1)
    plane_tails(u1, ts1)
    ls[0] = first_of(u1, 0, (0, 7))
    ls[1] = last_of(u1, 7, (0, 7))
    for m in late_packs + planes1:
        m.start()

    sweep(u1, False, (1, 6), store_wide)
    move(NEXT)
    for m in moves[NEXT]:
        m.start()
    for part in (INNER, MIDDLE, EDGE_LOW, EDGE_HIGH):
        finish(part, drift_prev, drift_next)

    for m in late_packs:
        m.wait_recv()
    fill_x(u1, jnp.where(has_left, lr[0], zero), jnp.where(has_right, lr[1], zero), (0, 7))
    for m in planes1[:3]:
        m.wait_recv()
    halos(rx1, drift_prev, (1,))
    for part in (HIGH_A, HIGH_B):
        sweep(u1, False, (7,), store_wide, (part[2], part[2] + 4, 2))
        move(part)
        for m in moves[part]:
            m.start()
    for m in planes1[3:]:
        m.wait_recv()
    halos(rx1, drift_prev, (0,))
    for part in (LOW_A, LOW_B):
        sweep(u1, False, (0,), store_wide, (part[2], part[2] + 4, 2))
        move(part)
        for m in moves[part]:
            m.start()
    for part in (NEXT, HIGH_A, HIGH_B, LOW_A, LOW_B):
        finish(part, drift_prev, drift_next)

    for m in packs + count_x + count_z + planes0 + count_g + late_packs + planes1:
        m.wait_send()
    for part in PARTS:
        for m in moves[part]:
            m.wait_send()


N_MESSAGES = (NX - 1) + (NZ - 1) + 2 + 2 + 2 + 6 + 6 + 2 * len(PARTS)


def local(state, coef, counts):
    f32, i32 = jnp.float32, jnp.int32
    vmem = pltpu.VMEM
    result = pl.pallas_call(
        kernel,
        out_shape=vmem((8, 8, 64, 128), f32),
        in_specs=[
            pl.BlockSpec(memory_space=pltpu.SMEM),
            pl.BlockSpec(memory_space=pl.ANY),
            pl.BlockSpec(memory_space=pl.ANY),
        ],
        out_specs=pl.BlockSpec(memory_space=vmem),
        scratch_shapes=[
            vmem((8, 8, 96, 128), f32), vmem((8, 8, 96, 128), f32), vmem((8, 8, 96, 128), f32),
            vmem((10, 8, CH, 8, 128), f32), vmem((10, 8, CH, 8, 128), f32), vmem((8, 8, CH, 8, 128), f32),
            vmem((2, 8, CH, 8, 128), f32),
            vmem((8, 25, 8, 128), f32), vmem((8, 25, 8, 128), f32), vmem((8, 25, 8, 128), f32), vmem((8, 25, 8, 128), f32),
            vmem((2, 8, 4, 8, 128), f32), vmem((2, 8, 4, 8, 128), f32),
            vmem((2, 4, 8, 128), f32), vmem((2, 4, 8, 128), f32),
            vmem((2, 8, 128), f32), vmem((2, 8, 128), f32),
            vmem((8, 8, 2, 8, 128), f32), vmem((8, 8, 2, 8, 128), f32),
            vmem((8, 8, 2, 8, 128), f32), vmem((8, 8, 2, 8, 128), f32),
            vmem((8, 8, 17, 8, 128), f32),
            vmem((NX, 1, 128), i32), vmem((NZ, NX, 1, 128), i32), vmem((2, 8, 128), i32), vmem((1, 128), i32), vmem((8, 128), i32),
            pltpu.SemaphoreType.DMA((3, 8)),
            pltpu.SemaphoreType.DMA((N_MESSAGES,)), pltpu.SemaphoreType.DMA((N_MESSAGES,)),
        ],
        compiler_params=pltpu.CompilerParams(
            collective_id=0, has_side_effects=True, vmem_limit_bytes=60 * 1024 * 1024),
    )(counts, state.reshape(2, 8, 8, 96, 128), coef.reshape(8, 8, 96, 128))
    return result.reshape(512, 1, AVG)


def solution(mesh):
    placed = (P(None, None, "grp", "curve"), P(None, "grp", "curve"), P("grp", "curve"))
    return jax.shard_map(
        local, mesh=mesh, in_specs=placed, out_specs=P(None, "grp", "curve"), check_vma=False
    )
```
